256 devices in a mesh: stream: 32 (over y_hi, z, core), tm: 8 (over x, y_lo).
Axes of the slice: x: 4, y: 4 (y_hi: 2, y_lo: 2; y = y_hi * 2 + y_lo), z: 8, core: 2. Of those that a mesh axis runs over, the one named last changes fastest.
Arguments:
- signal: bfloat16 [64, 2, 4194304], P('stream', None, 'tm'), parts along dimension 0, may hold values from -11 to 11
- taps: float32 [16, 4096], replicated, may hold values from -1.5 to 1.5
Outputs:
- channels_out: float32 [64, 2, 4096, 1024], P('stream', None, 'tm'), parts along dimension 0
The draws below stay inside these ranges and needn't reach their ends.
There are 32 independent parts, one for each index of `stream`. The reference program is written for one: setup_inputs(seed, part) draws one part's arguments, and reference() takes and returns one part's arrays. A program takes and returns all parts, laid end to end along the dimension named above; an argument that names none is the same for every part. Nothing has to cross between parts.
All inputs are finite; a program needn't handle non-finite values.
Results may differ from the reference program's by a relative error of at most 0.0003.
Values may be sent and summed in bfloat16 or wider, within the bound.
A program may use at most 128 MiB of HBM per device.

```python
import math
import jax
import jax.numpy as jnp
from jax import lax

CHANNELS = 4096
RADIX = 64
TAPS = 16
STREAMS = 2
FRAMES = 1024
SAMPLES = 4194304


def draw_signal(key, part):
    key_noise, key_gain, key_freq, key_level = jax.random.split(key, 4)
    blocks = FRAMES // 8 + 1
    position = jnp.arange(SAMPLES, dtype=jnp.int32)
    which = position // CHANNELS // 8
    noise = jax.random.truncated_normal(key_noise, -4.0, 4.0, (STREAMS, 2, SAMPLES), jnp.float32)
    gains = jnp.exp(jax.random.uniform(key_gain, (STREAMS, blocks), jnp.float32, math.log(0.5), math.log(2.0)))
    envelope = gains[:, which]
    numerators = jax.random.randint(key_freq, (STREAMS, 3), 0, 1 << 20, jnp.int32)
    levels = jax.random.uniform(key_level, (STREAMS, 3), jnp.float32, 0.3, 1.0)
    tone_real = jnp.zeros((STREAMS, SAMPLES), jnp.float32)
    tone_imag = jnp.zeros((STREAMS, SAMPLES), jnp.float32)
    for number in range(3):
        wrapped = jnp.bitwise_and(numerators[:, number][:, None] * position[None, :], (1 << 20) - 1)
        phase = wrapped.astype(jnp.float32) * (2.0 * math.pi / (1 << 20))
        tone_real = tone_real + levels[:, number][:, None] * jnp.cos(phase)
        tone_imag = tone_imag + levels[:, number][:, None] * jnp.sin(phase)
    result = jnp.stack([noise[:, 0] * envelope + tone_real, noise[:, 1] * envelope + tone_imag], axis=1)
    return result.astype(jnp.bfloat16)


def bell_draw(rng, shape, scale, bound, held_as=jnp.bfloat16):
    array = jax.random.normal(rng, shape, jnp.float32) * scale
    return jnp.minimum(jnp.maximum(array, -bound), bound).astype(held_as)


def setup_inputs(seed: int = 0, part: int = 0) -> dict:
    key_of = jax.random.split(jax.random.key(seed), 3)
    part_keys = jax.random.split(jax.random.fold_in(key_of[2], part), 3)
    signal = draw_signal(jax.random.fold_in(jax.random.fold_in(key_of[2], part), 71), part)
    taps = bell_draw(key_of[1], (TAPS, CHANNELS), TAPS ** -0.5, 1.5, jnp.float32)
    return {"signal": signal, "taps": taps}


def reference(signal, taps):
    streams = signal.shape[0]
    frames = signal.astype(jnp.float32).reshape(streams, 2, FRAMES, CHANNELS)
    padded = jnp.pad(frames, ((0, 0), (0, 0), (TAPS - 1, 0), (0, 0)))
    filtered = jnp.zeros((streams, 2, FRAMES, CHANNELS), jnp.float32)
    for tap_index in range(TAPS):
        start = TAPS - 1 - tap_index
        filtered = filtered + taps[tap_index] * padded[:, :, start:start + FRAMES, :]
    spectrum = jnp.fft.fft(lax.complex(filtered[:, 0], filtered[:, 1]), axis=-1) / RADIX
    real_part = jnp.real(spectrum)
    imag_part = jnp.imag(spectrum)
    power = lax.optimization_barrier(jnp.mean(real_part * real_part + imag_part * imag_part, axis=1))
    factor = 1.0 / jnp.sqrt(power + 1.0)
    stacked = jnp.stack([real_part * factor[:, None, :], imag_part * factor[:, None, :]], axis=1)
    return jnp.transpose(stacked, (0, 1, 3, 2))
```

```python
import math

import jax
import jax.numpy as jnp
import numpy as np
from jax import lax
from jax.experimental import pallas as pl
from jax.experimental.pallas import tpu as pltpu
from jax.sharding import PartitionSpec as P

MESH = pl.DeviceIdType.MESH
F32 = jnp.float32
BF16 = jnp.bfloat16

LANES = 128
FIRST = 32
HALF = 16
TAPS_PITCH = 72
FRAME_PITCH = 72
CHANNEL_PITCH = 24
SPAN = 125.0
PEERS = ((2, 1), (2, 0), (1, 1), (3, 1), (0, 1), (1, 0), (3, 0))


def section_table():
    index = np.arange(LANES)
    angle = 2.0 * math.pi * (np.outer(index, index) % LANES) / LANES
    cos, sin = np.cos(angle) / 64.0, np.sin(angle) / 64.0
    return np.block([[cos, sin], [-sin, cos]]).astype(np.float32)


def twist_tables():
    angle = 2.0 * math.pi * np.outer(np.arange(FIRST), np.arange(LANES)) / (FIRST * LANES)
    return np.cos(angle).astype(np.float32), np.sin(angle).astype(np.float32)


def plus(a, b):
    return a[0] + b[0], a[1] + b[1]


def minus(a, b):
    return a[0] - b[0], a[1] - b[1]


def minus_i(a):
    return a[1], -a[0]


def turned(a, step, points):
    step %= points
    if step == 0:
        return a
    if step * 4 == points:
        return a[1], -a[0]
    if step * 2 == points:
        return -a[0], -a[1]
    if step * 8 == points:
        c = np.float32(math.sqrt(0.5))
        return (a[0] + a[1]) * c, (a[1] - a[0]) * c
    if step * 8 == 3 * points:
        c = np.float32(math.sqrt(0.5))
        return (a[1] - a[0]) * c, (a[0] + a[1]) * -c
    c = np.float32(math.cos(2.0 * math.pi * step / points))
    s = np.float32(math.sin(2.0 * math.pi * step / points))
    return a[0] * c + a[1] * s, a[1] * c - a[0] * s


def four(v):
    a, b = plus(v[0], v[2]), minus(v[0], v[2])
    c, d = plus(v[1], v[3]), minus_i(minus(v[1], v[3]))
    return [plus(a, c), plus(b, d), minus(a, c), minus(b, d)]


def eight(v):
    even, odd = four(v[0::2]), four(v[1::2])
    odd = [turned(odd[i], i, 8) for i in range(4)]
    return [plus(even[i], odd[i]) for i in range(4)] + [minus(even[i], odd[i]) for i in range(4)]


def first_section(load):
    parts = [[None] * 8 for _ in range(4)]
    for b in range(8):
        column = four([load(8 * a + b) for a in range(4)])
        for p in range(4):
            parts[p][b] = turned(column[p], b * p, FIRST)
    out = [None] * FIRST
    for p in range(4):
        for q, value in enumerate(eight(parts[p])):
            out[p + 4 * q] = value
    return out


def transposed_dot(a, b):
    return lax.dot_general(a, b, (((1,), (1,)), ((), ())), preferred_element_type=F32)


def channelize(streams, frames, ways, z_ref, taps_ref, high_ref, low_ref, cos_ref, sin_ref, got_ref, scales_ref,
               x_ref, taps_scr, frame_scr, grid_scr, channel_scr, send_ref, table_scr, table_ref,
               load_sem, halo_send, halo_recv, send_sem, recv_sem, table_send, table_recv, own_sem, own_table_sem):
    rows = 2 * FIRST
    halo = 16 * rows
    edge = 15 * rows
    own = LANES // ways
    me = lax.axis_index("tm")
    across, along = me // 2, lax.rem(me, 2)

    def peer_of(number):
        dx, dy = PEERS[number]
        return lax.rem(across + dx, ways // 2) * 2 + lax.rem(along + dy, 2)

    barrier = pltpu.get_barrier_semaphore()
    for number in range(ways - 1):
        pl.semaphore_signal(barrier, inc=1, device_id={"tm": peer_of(number)}, device_id_type=MESH)

    def load(s):
        return pltpu.make_async_copy(z_ref.at[s], x_ref.at[s, pl.ds(halo, frames * rows), :], load_sem.at[s])

    def pass_on(s):
        return pltpu.make_async_remote_copy(
            src_ref=z_ref.at[s, pl.ds(frames * rows - edge, edge), :],
            dst_ref=x_ref.at[s, pl.ds(halo - edge, edge), :],
            send_sem=halo_send.at[s],
            recv_sem=halo_recv.at[s],
            device_id={"tm": lax.rem(me + 1, ways)},
            device_id_type=MESH,
        )

    for s in range(streams):
        load(s).start()
    pl.semaphore_wait(barrier, ways - 1)

    @pl.when(me < ways - 1)
    def _():
        for s in range(streams):
            pass_on(s).start()

    @pl.when(me == 0)
    def _():
        for s in range(streams):
            x_ref[s, pl.ds(halo - edge, edge), :] = jnp.zeros((edge, LANES), BF16)

    for octet in range(2):
        for m1 in range(FIRST):
            block = taps_ref[pl.ds(8 * octet, 8), pl.ds(LANES * m1, LANES)]
            for part in range(2):
                taps_scr[pl.ds(8 * octet * TAPS_PITCH + 2 * m1 + part, 8, stride=TAPS_PITCH), :] = block

    lane = lax.broadcasted_iota(jnp.int32, (LANES, LANES), 1)

    def transform(s, tb):
        for g in range(rows // 16):
            total = [None] * 8
            for j in range(23):
                start = pl.multiple_of((8 * tb + 1 + j) * rows + 16 * g, 16)
                x = x_ref[s, pl.ds(start, 16), :].astype(F32)
                for o in range(8):
                    k = o + 15 - j
                    if 0 <= k < 16:
                        term = taps_scr[k * TAPS_PITCH + 16 * g : k * TAPS_PITCH + 16 * g + 16, :] * x
                        total[o] = term if total[o] is None else total[o] + term
            for o in range(8):
                frame_scr[o * FRAME_PITCH + 16 * g : o * FRAME_PITCH + 16 * g + 16, :] = total[o]

        def fetch(m1):
            return tuple(frame_scr[pl.ds(2 * m1 + part, 8, stride=FRAME_PITCH), :] for part in range(2))

        at = pl.ds(pl.multiple_of(8 * tb, 8), 8)
        for c1, (real, imag) in enumerate(first_section(fetch)):
            cos, sin = cos_ref[c1 : c1 + 1, :], sin_ref[c1 : c1 + 1, :]
            grid_scr[c1, at, 0:LANES] = real * cos + imag * sin
            grid_scr[c1, at, LANES : 2 * LANES] = imag * cos - real * sin

    def outgoing(s, h, number):
        peer = peer_of(number)
        return pltpu.make_async_remote_copy(
            src_ref=send_ref.at[s, h, peer],
            dst_ref=got_ref.at[s, h, me],
            send_sem=send_sem.at[s, h, number],
            recv_sem=recv_sem.at[s, h, me],
            device_id={"tm": peer},
            device_id_type=MESH,
        )

    def outgoing_table(s, number):
        peer = peer_of(number)
        return pltpu.make_async_remote_copy(
            src_ref=table_ref.at[s, pl.ds(pl.multiple_of(peer * own, own), own), :],
            dst_ref=scales_ref.at[s, me],
            send_sem=table_send.at[s, number],
            recv_sem=table_recv.at[s, me],
            device_id={"tm": peer},
            device_id_type=MESH,
        )

    def own_block(s, h):
        return pltpu.make_async_copy(send_ref.at[s, h, me], got_ref.at[s, h, me], own_sem.at[s, h])

    def own_table(s):
        return pltpu.make_async_copy(
            table_ref.at[s, pl.ds(pl.multiple_of(me * own, own), own), :], scales_ref.at[s, me], own_table_sem.at[s]
        )

    def incoming(s, h, number):
        peer = peer_of(number)
        return pltpu.make_async_remote_copy(
            src_ref=send_ref.at[s, h, peer],
            dst_ref=got_ref.at[s, h, peer],
            send_sem=send_sem.at[s, h, number],
            recv_sem=recv_sem.at[s, h, peer],
            device_id={"tm": peer},
            device_id_type=MESH,
        )

    def incoming_table(s, number):
        peer = peer_of(number)
        return pltpu.make_async_remote_copy(
            src_ref=table_ref.at[s, pl.ds(pl.multiple_of(peer * own, own), own), :],
            dst_ref=scales_ref.at[s, peer],
            send_sem=table_send.at[s, number],
            recv_sem=table_recv.at[s, peer],
            device_id={"tm": peer},
            device_id_type=MESH,
        )

    def second_section(h, place):
        c1 = h * HALF + place
        y = grid_scr[c1]
        high = y.astype(BF16)
        low = (y - high.astype(F32)).astype(BF16)
        wide = transposed_dot(high_ref[...], jnp.concatenate([high, low], axis=0))
        value = wide[:, :LANES] + wide[:, LANES:] + transposed_dot(low_ref[...], high)
        real, imag = value[:LANES], value[LANES:]
        power = jnp.sum(real * real + imag * imag, axis=1, keepdims=True)
        largest = jnp.max(jnp.maximum(jnp.abs(real), jnp.abs(imag)), axis=1, keepdims=True)
        largest = (largest * np.float32(1.0 + 2.0**-7)).astype(BF16).astype(F32)
        largest = jnp.maximum(largest, np.float32(2.0**-96))
        power_high = power.astype(BF16).astype(F32)
        mine = jnp.where(lane < FIRST, largest, jnp.where(lane < 2 * FIRST, power_high, power - power_high))
        table_scr[...] = jnp.where(lax.rem(lane, FIRST) == c1, mine, table_scr[...])
        scale = SPAN / largest
        for part, piece in enumerate((real, imag)):
            coded = jnp.exp2(piece * scale)
            for c in range(0, LANES, 8):
                channel_scr[part, pl.ds(c * CHANNEL_PITCH + place, 8, stride=CHANNEL_PITCH), :] = coded[c : c + 8]

    def pack(s, h, d):
        for part in range(2):
            for j in range(own):
                start = pl.multiple_of((d * own + j) * CHANNEL_PITCH, 8)
                send_ref[s, h, d, part, j * HALF : (j + 1) * HALF, :] = channel_scr[part, pl.ds(start, HALF), :].astype(BF16)

    blocks = frames // 8

    def one_stream(s, carry):
        load(s).wait()
        lax.fori_loop(2, blocks, lambda tb, c: (transform(s, tb), c)[1], 0)

        @pl.when(me > 0)
        def _():
            pass_on(s).wait_recv()

        lax.fori_loop(0, 2, lambda tb, c: (transform(s, tb), c)[1], 0)
        table_scr[...] = jnp.zeros((LANES, LANES), F32)

        def one_half(h, carry):
            lax.fori_loop(0, HALF, lambda place, c: (second_section(h, place), c)[1], 0)
            lax.fori_loop(0, ways, lambda d, c: (pack(s, h, d), c)[1], 0)
            for number in range(ways - 1):
                outgoing(s, h, number).start()
            own_block(s, h).start()
            return carry

        lax.fori_loop(0, FIRST // HALF, one_half, 0)
        table_ref[s] = table_scr[...].astype(BF16)
        for number in range(ways - 1):
            outgoing_table(s, number).start()
        own_table(s).start()
        return carry

    lax.fori_loop(0, streams, one_stream, 0)

    @pl.when(me < ways - 1)
    def _():
        for s in range(streams):
            pass_on(s).wait_send()

    def finish(s, carry):
        for h in range(FIRST // HALF):
            for number in range(ways - 1):
                outgoing(s, h, number).wait_send()
                incoming(s, h, number).wait_recv()
            own_block(s, h).wait()
        for number in range(ways - 1):
            outgoing_table(s, number).wait_send()
            incoming_table(s, number).wait_recv()
        own_table(s).wait()
        return carry

    lax.fori_loop(0, streams, finish, 0)


def equalize(frames, ways, group, got_ref, scales_ref, out_ref, factor_scr):
    own = LANES // ways

    @pl.when(pl.program_id(1) == 0)
    def _():
        table = scales_ref[0].reshape(ways * own, LANES).astype(F32).T
        largest, power = table[:FIRST], table[FIRST : 2 * FIRST] + table[2 * FIRST : 3 * FIRST]
        step = LANES // 2
        while step >= own:
            power = power + pltpu.roll(power, step, 1)
            step //= 2
        mean = power * np.float32(1.0 / (frames * ways))
        factor_scr[...] = largest * np.float32(math.log2(math.e) / SPAN) * lax.rsqrt(mean + 1.0)

    first = pl.program_id(1) * group
    factors = pltpu.roll(factor_scr[...], lax.rem(LANES - first, LANES), 1)
    for j in range(group):
        for way in range(ways):
            for h in range(FIRST // HALF):
                factor = factors[h * HALF : (h + 1) * HALF, way * own + j : way * own + j + 1]
                for part in range(2):
                    coded = got_ref[0, h, way, part, j * HALF : (j + 1) * HALF, :].astype(F32)
                    row = j * FIRST + h * HALF
                    out_ref[0, part, row : row + HALF, way * LANES : (way + 1) * LANES] = jnp.log(coded) * factor


def shards(signal, taps):
    streams, _, samples = signal.shape
    channels = taps.shape[1]
    ways = lax.axis_size("tm")
    frames = samples // channels
    rows = 2 * FIRST
    own = LANES // ways
    z = signal.reshape(streams, 2, samples // LANES, LANES).transpose(0, 2, 1, 3).reshape(streams, frames * rows, LANES)
    table = section_table()
    high = table.astype(jnp.bfloat16)
    low = (table - high.astype(np.float32)).astype(jnp.bfloat16)
    cos, sin = twist_tables()
    vmem = pl.BlockSpec(memory_space=pltpu.VMEM)
    hbm = pl.BlockSpec(memory_space=pltpu.HBM)
    halves = FIRST // HALF
    dma = pltpu.SemaphoreType.DMA
    got, scales = pl.pallas_call(
        lambda *refs: channelize(streams, frames, ways, *refs),
        out_shape=(
            jax.ShapeDtypeStruct((streams, halves, ways, 2, own * HALF, LANES), BF16),
            jax.ShapeDtypeStruct((streams, ways, own, LANES), BF16),
        ),
        in_specs=[hbm, vmem, vmem, vmem, vmem, vmem],
        out_specs=(hbm, hbm),
        scratch_shapes=[
            pltpu.VMEM((streams, (frames + 16) * rows, LANES), BF16),
            pltpu.VMEM((16 * TAPS_PITCH, LANES), F32),
            pltpu.VMEM((8 * FRAME_PITCH, LANES), F32),
            pltpu.VMEM((FIRST, frames, 2 * LANES), F32),
            pltpu.VMEM((2, LANES * CHANNEL_PITCH, LANES), F32),
            pltpu.VMEM((streams, halves, ways, 2, own * HALF, LANES), BF16),
            pltpu.VMEM((LANES, LANES), F32),
            pltpu.VMEM((streams, LANES, LANES), BF16),
            dma((streams,)),
            dma((streams,)),
            dma((streams,)),
            dma((streams, halves, ways)),
            dma((streams, halves, ways)),
            dma((streams, ways)),
            dma((streams, ways)),
            dma((streams, halves)),
            dma((streams,)),
        ],
        compiler_params=pltpu.CompilerParams(collective_id=0, has_side_effects=True, vmem_limit_bytes=48 << 20),
        name="channelize",
    )(z, taps, jnp.asarray(high), jnp.asarray(low), jnp.asarray(cos), jnp.asarray(sin))
    group = 4
    return pl.pallas_call(
        lambda *refs: equalize(frames, ways, group, *refs),
        grid=(streams, own // group),
        out_shape=jax.ShapeDtypeStruct((streams, 2, channels // ways, frames * ways), F32),
        in_specs=[
            pl.BlockSpec((1, halves, ways, 2, group * HALF, LANES), lambda s, j: (s, 0, 0, 0, j, 0)),
            pl.BlockSpec((1, ways, own, LANES), lambda s, j: (s, 0, 0, 0)),
        ],
        out_specs=pl.BlockSpec((1, 2, group * FIRST, frames * ways), lambda s, j: (s, 0, j, 0)),
        scratch_shapes=[pltpu.VMEM((FIRST, LANES), F32)],
        compiler_params=pltpu.CompilerParams(dimension_semantics=("arbitrary", "arbitrary")),
        name="equalize",
    )(got, scales)


def solution(mesh):
    in_specs = (P("stream", None, "tm"), P())
    out_specs = P("stream", None, "tm", None)
    return jax.shard_map(shards, mesh=mesh, in_specs=in_specs, out_specs=out_specs, check_vma=False)
```

```python
import math

import jax
import jax.numpy as jnp
import numpy as np
from jax import lax
from jax.experimental import pallas as pl
from jax.experimental.pallas import tpu as pltpu
from jax.sharding import PartitionSpec as P

MESH = pl.DeviceIdType.MESH
F32 = jnp.float32
BF16 = jnp.bfloat16

LANES = 128
FIRST = 32
GROUP = 8
TAPS_PITCH = 72
FRAME_PITCH = 72
UNROLL = 4
PART_ROWS = 4
SPAN = 125.0
PEERS = ((2, 1), (2, 0), (1, 1), (3, 1), (0, 1), (1, 0), (3, 0))


def constant_table():
    index = np.arange(LANES)
    angle = 2.0 * math.pi * (np.outer(index, index) % LANES) / LANES
    cos, sin = np.cos(angle) / 64.0, np.sin(angle) / 64.0
    matrix = np.block([[cos, sin], [-sin, cos]])
    high = matrix.astype(jnp.bfloat16).astype(np.float64)
    twist = 2.0 * math.pi * np.outer(np.arange(FIRST), index) / (FIRST * LANES)
    return np.concatenate([high, matrix - high, np.concatenate([np.cos(twist), np.sin(twist)], axis=1)]).astype(np.float32)


def plus(a, b):
    return a[0] + b[0], a[1] + b[1]


def minus(a, b):
    return a[0] - b[0], a[1] - b[1]


def minus_i(a):
    return a[1], -a[0]


def turned(a, step, points):
    step %= points
    if step == 0:
        return a
    if step * 4 == points:
        return a[1], -a[0]
    if step * 2 == points:
        return -a[0], -a[1]
    if step * 8 == points:
        c = np.float32(math.sqrt(0.5))
        return (a[0] + a[1]) * c, (a[1] - a[0]) * c
    if step * 8 == 3 * points:
        c = np.float32(math.sqrt(0.5))
        return (a[1] - a[0]) * c, (a[0] + a[1]) * -c
    c = np.float32(math.cos(2.0 * math.pi * step / points))
    s = np.float32(math.sin(2.0 * math.pi * step / points))
    return a[0] * c + a[1] * s, a[1] * c - a[0] * s


def four(v):
    a, b = plus(v[0], v[2]), minus(v[0], v[2])
    c, d = plus(v[1], v[3]), minus_i(minus(v[1], v[3]))
    return [plus(a, c), plus(b, d), minus(a, c), minus(b, d)]


def eight(v):
    even, odd = four(v[0::2]), four(v[1::2])
    odd = [turned(odd[i], i, 8) for i in range(4)]
    return [plus(even[i], odd[i]) for i in range(4)] + [minus(even[i], odd[i]) for i in range(4)]


def first_section(load):
    parts = [[None] * 8 for _ in range(4)]
    for b in range(8):
        column = four([load(8 * a + b) for a in range(4)])
        for p in range(4):
            parts[p][b] = turned(column[p], b * p, FIRST)
    out = [None] * FIRST
    for p in range(4):
        for q, value in enumerate(eight(parts[p])):
            out[p + 4 * q] = value
    return out


def transposed_dot(a, b):
    return lax.dot_general(a, b, (((1,), (1,)), ((), ())), preferred_element_type=F32)


def channelize(streams, frames, ways, z_ref, taps_in, constants_in, got_ref, scales_ref,
               taps_ref, constants_ref, matrix_ref, x_ref, taps_scr, frame_scr, grid_scr, channel_scr, send_ref, table_scr, table_ref,
               table_load, load_sem, halo_send, halo_recv, send_sem, recv_sem, table_send, table_recv, own_sem, own_table_sem):
    rows = 2 * FIRST
    halo = 16 * rows
    edge = 15 * rows
    own = LANES // ways
    me = lax.axis_index("tm")
    across, along = me // 2, lax.rem(me, 2)

    def peer_of(number):
        dx, dy = PEERS[number]
        return lax.rem(across + dx, ways // 2) * 2 + lax.rem(along + dy, 2)

    barrier = pltpu.get_barrier_semaphore()
    for number in range(ways - 1):
        pl.semaphore_signal(barrier, inc=1, device_id={"tm": peer_of(number)}, device_id_type=MESH)

    def load(s):
        return pltpu.make_async_copy(z_ref.at[s], x_ref.at[s, pl.ds(halo, frames * rows), :], load_sem.at[s])

    def pass_on(s):
        return pltpu.make_async_remote_copy(
            src_ref=z_ref.at[s, pl.ds(frames * rows - edge, edge), :],
            dst_ref=x_ref.at[s, pl.ds(halo - edge, edge), :],
            send_sem=halo_send.at[s],
            recv_sem=halo_recv.at[s],
            device_id={"tm": lax.rem(me + 1, ways)},
            device_id_type=MESH,
        )

    tables = [
        pltpu.make_async_copy(taps_in, taps_ref, table_load.at[0]),
        pltpu.make_async_copy(constants_in, constants_ref, table_load.at[1]),
    ]
    tables[0].start()
    for s in range(streams):
        load(s).start()
    tables[1].start()
    pl.semaphore_wait(barrier, ways - 1)

    @pl.when(me < ways - 1)
    def _():
        for s in range(streams):
            pass_on(s).start()

    @pl.when(me == 0)
    def _():
        for s in range(streams):
            x_ref[s, pl.ds(halo - edge, edge), :] = jnp.zeros((edge, LANES), BF16)

    for copy in tables:
        copy.wait()
    for row in range(0, 4 * LANES, 64):
        matrix_ref[row : row + 64, :] = constants_ref[row : row + 64, :].astype(BF16)
    for octet in range(2):
        for m1 in range(FIRST):
            block = taps_ref[pl.ds(8 * octet, 8), pl.ds(LANES * m1, LANES)]
            for part in range(2):
                taps_scr[pl.ds(8 * octet * TAPS_PITCH + 2 * m1 + part, 8, stride=TAPS_PITCH), :] = block

    lane = lax.broadcasted_iota(jnp.int32, (LANES, LANES), 1)
    lane_c1 = lax.bitwise_and(lane, FIRST - 1)

    def transform(s, tb):
        for g in range(rows // 16):
            total = [None] * 8
            for j in range(23):
                start = pl.multiple_of((8 * tb + 1 + j) * rows + 16 * g, 16)
                x = x_ref[s, pl.ds(start, 16), :].astype(F32)
                for o in range(8):
                    k = o + 15 - j
                    if 0 <= k < 16:
                        term = taps_scr[k * TAPS_PITCH + 16 * g : k * TAPS_PITCH + 16 * g + 16, :] * x
                        total[o] = term if total[o] is None else total[o] + term
            for o in range(8):
                frame_scr[o * FRAME_PITCH + 16 * g : o * FRAME_PITCH + 16 * g + 16, :] = total[o]

        def fetch(m1):
            return tuple(frame_scr[pl.ds(2 * m1 + part, 8, stride=FRAME_PITCH), :] for part in range(2))

        at = pl.ds(pl.multiple_of(8 * tb, 8), 8)
        for c1, (real, imag) in enumerate(first_section(fetch)):
            cos, sin = (constants_ref[4 * LANES + c1 : 4 * LANES + c1 + 1, k * LANES : (k + 1) * LANES] for k in range(2))
            grid_scr[c1, at, 0:LANES] = real * cos + imag * sin
            grid_scr[c1, at, LANES : 2 * LANES] = imag * cos - real * sin

    def outgoing(s, h, number):
        peer = peer_of(number)
        return pltpu.make_async_remote_copy(
            src_ref=send_ref.at[s, h, peer],
            dst_ref=got_ref.at[s, h, me],
            send_sem=send_sem.at[s, h, number],
            recv_sem=recv_sem.at[s, h, me],
            device_id={"tm": peer},
            device_id_type=MESH,
        )

    def outgoing_table(s, number):
        peer = peer_of(number)
        return pltpu.make_async_remote_copy(
            src_ref=table_ref.at[s, pl.ds(pl.multiple_of(peer * own, own), own), :],
            dst_ref=scales_ref.at[s, me],
            send_sem=table_send.at[s, number],
            recv_sem=table_recv.at[s, me],
            device_id={"tm": peer},
            device_id_type=MESH,
        )

    def own_block(s, h):
        return pltpu.make_async_copy(send_ref.at[s, h, me], got_ref.at[s, h, me], own_sem.at[s, h])

    def own_table(s):
        return pltpu.make_async_copy(
            table_ref.at[s, pl.ds(pl.multiple_of(me * own, own), own), :], scales_ref.at[s, me], own_table_sem.at[s]
        )

    def incoming(s, h, number):
        peer = peer_of(number)
        return pltpu.make_async_remote_copy(
            src_ref=send_ref.at[s, h, peer],
            dst_ref=got_ref.at[s, h, peer],
            send_sem=send_sem.at[s, h, number],
            recv_sem=recv_sem.at[s, h, peer],
            device_id={"tm": peer},
            device_id_type=MESH,
        )

    def incoming_table(s, number):
        peer = peer_of(number)
        return pltpu.make_async_remote_copy(
            src_ref=table_ref.at[s, pl.ds(pl.multiple_of(peer * own, own), own), :],
            dst_ref=scales_ref.at[s, peer],
            send_sem=table_send.at[s, number],
            recv_sem=table_recv.at[s, peer],
            device_id={"tm": peer},
            device_id_type=MESH,
        )

    def second_section(h, place):
        c1 = h * GROUP + place
        y = grid_scr[c1]
        high = y.astype(BF16)
        low = (y - high.astype(F32)).astype(BF16)
        wide = transposed_dot(matrix_ref[: 2 * LANES], jnp.concatenate([high, low], axis=0))
        value = wide[:, :LANES] + wide[:, LANES:] + transposed_dot(matrix_ref[2 * LANES :], high)
        real, imag = value[:LANES], value[LANES:]
        power = jnp.sum(real * real + imag * imag, axis=1, keepdims=True)
        largest = jnp.max(jnp.maximum(jnp.abs(real), jnp.abs(imag)), axis=1, keepdims=True)
        largest = (largest * np.float32(1.0 + 2.0**-7)).astype(BF16).astype(F32)
        largest = jnp.maximum(largest, np.float32(2.0**-96))
        power_high = power.astype(BF16).astype(F32)
        mine = jnp.where(lane < FIRST, largest, jnp.where(lane < 2 * FIRST, power_high, power - power_high))
        table_scr[...] = jnp.where(lane_c1 == c1, mine, table_scr[...])
        scale = SPAN / largest
        for part, piece in enumerate((real, imag)):
            coded = jnp.exp2(piece * scale)
            for c in range(0, LANES, 8):
                channel_scr[part, pl.ds(c * GROUP + place, 8, stride=GROUP), :] = coded[c : c + 8]

    def pack(s, h, d):
        for part in range(2):
            for row in range(0, own * GROUP, 16):
                start = pl.multiple_of(d * own * GROUP + row, 16)
                send_ref[s, h, d, part, row : row + 16, :] = channel_scr[part, pl.ds(start, 16), :].astype(BF16)

    blocks = frames // 8

    def one_stream(s, carry):
        load(s).wait()
        lax.fori_loop(2, blocks, lambda tb, c: (transform(s, tb), c)[1], 0)

        @pl.when(me > 0)
        def _():
            pass_on(s).wait_recv()

        lax.fori_loop(0, 2, lambda tb, c: (transform(s, tb), c)[1], 0)
        table_scr[...] = jnp.zeros((LANES, LANES), F32)

        def one_group(h, carry):
            lax.fori_loop(0, GROUP, lambda place, c: (second_section(h, place), c)[1], 0, unroll=UNROLL)
            lax.fori_loop(0, ways, lambda d, c: (pack(s, h, d), c)[1], 0)
            for number in range(ways - 1):
                outgoing(s, h, number).start()
            own_block(s, h).start()
            return carry

        lax.fori_loop(0, FIRST // GROUP, one_group, 0)
        table_ref[s] = table_scr[...].astype(BF16)
        for number in range(ways - 1):
            outgoing_table(s, number).start()
        own_table(s).start()
        return carry

    lax.fori_loop(0, streams, one_stream, 0)

    @pl.when(me < ways - 1)
    def _():
        for s in range(streams):
            pass_on(s).wait_send()

    def finish(s, carry):
        for h in range(FIRST // GROUP):
            for number in range(ways - 1):
                outgoing(s, h, number).wait_send()
                incoming(s, h, number).wait_recv()
            own_block(s, h).wait()
        for number in range(ways - 1):
            outgoing_table(s, number).wait_send()
            incoming_table(s, number).wait_recv()
        own_table(s).wait()
        return carry

    lax.fori_loop(0, streams, finish, 0)


def equalize(streams, frames, ways, part_rows, got_ref, scales_ref, out_ref, factor_scr, out_scr, sem):
    own = LANES // ways
    parts = own // part_rows
    for s in range(streams):
        table = scales_ref[s].reshape(ways * own, LANES).astype(F32).T
        largest, power = table[:FIRST], table[FIRST : 2 * FIRST] + table[2 * FIRST : 3 * FIRST]
        step = LANES // 2
        while step >= own:
            power = power + pltpu.roll(power, step, 1)
            step //= 2
        mean = power * np.float32(1.0 / (frames * ways))
        factor_scr[s] = largest * np.float32(math.log2(math.e) / SPAN) * lax.rsqrt(mean + 1.0)

    def copy_out(s, n):
        rows = pl.ds(pl.multiple_of(n * part_rows * FIRST, part_rows * FIRST), part_rows * FIRST)
        return pltpu.make_async_copy(out_scr.at[s, :, rows, :], out_ref.at[s, :, rows, :], sem.at[s, n])

    def one_part(index, carry):
        s, n = index // parts, lax.rem(index, parts)
        first = n * part_rows
        factors = pltpu.roll(factor_scr[s], lax.rem(LANES - first, LANES), 1)
        for way in range(ways):
            for h in range(FIRST // GROUP):
                for j in range(0, part_rows, 2):
                    factor = [
                        factors[h * GROUP : (h + 1) * GROUP, way * own + i : way * own + i + 1] for i in (j, j + 1)
                    ]
                    for part in range(2):
                        start = pl.multiple_of((first + j) * GROUP, 16)
                        value = jnp.log(got_ref[s, h, way, part, pl.ds(start, 16), :].astype(F32))
                        for i in range(2):
                            row = pl.multiple_of((first + j + i) * FIRST + h * GROUP, GROUP)
                            piece = value[i * GROUP : (i + 1) * GROUP] * factor[i]
                            out_scr[s, part, pl.ds(row, GROUP), way * LANES : (way + 1) * LANES] = piece
        copy_out(s, n).start()
        return carry

    lax.fori_loop(0, streams * parts, one_part, 0)
    for s in range(streams):
        for n in range(parts):
            copy_out(s, n).wait()


def shards(signal, taps):
    streams, _, samples = signal.shape
    channels = taps.shape[1]
    ways = lax.axis_size("tm")
    frames = samples // channels
    rows = 2 * FIRST
    own = LANES // ways
    z = signal.reshape(streams, 2, samples // LANES, LANES).transpose(0, 2, 1, 3).reshape(streams, frames * rows, LANES)
    constants = constant_table()
    vmem = pl.BlockSpec(memory_space=pltpu.VMEM)
    hbm = pl.BlockSpec(memory_space=pltpu.HBM)
    groups = FIRST // GROUP
    dma = pltpu.SemaphoreType.DMA
    got, scales = pl.pallas_call(
        lambda *refs: channelize(streams, frames, ways, *refs),
        out_shape=(
            jax.ShapeDtypeStruct((streams, groups, ways, 2, own * GROUP, LANES), BF16),
            jax.ShapeDtypeStruct((streams, ways, own, LANES), BF16),
        ),
        in_specs=[hbm] * 3,
        out_specs=(vmem, vmem),
        scratch_shapes=[
            pltpu.VMEM(taps.shape, F32),
            pltpu.VMEM(constants.shape, F32),
            pltpu.VMEM((4 * LANES, 2 * LANES), BF16),
            pltpu.VMEM((streams, (frames + 16) * rows, LANES), BF16),
            pltpu.VMEM((16 * TAPS_PITCH, LANES), F32),
            pltpu.VMEM((8 * FRAME_PITCH, LANES), F32),
            pltpu.VMEM((FIRST, frames, 2 * LANES), F32),
            pltpu.VMEM((2, LANES * GROUP, LANES), F32),
            pltpu.VMEM((streams, groups, ways, 2, own * GROUP, LANES), BF16),
            pltpu.VMEM((LANES, LANES), F32),
            pltpu.VMEM((streams, LANES, LANES), BF16),
            dma((2,)),
            dma((streams,)),
            dma((streams,)),
            dma((streams,)),
            dma((streams, groups, ways)),
            dma((streams, groups, ways)),
            dma((streams, ways)),
            dma((streams, ways)),
            dma((streams, groups)),
            dma((streams,)),
        ],
        compiler_params=pltpu.CompilerParams(collective_id=0, has_side_effects=True, vmem_limit_bytes=48 << 20),
        name="channelize",
    )(z, taps, jnp.asarray(constants))
    part_rows = PART_ROWS
    out_shape = (streams, 2, channels // ways, frames * ways)
    return pl.pallas_call(
        lambda *refs: equalize(streams, frames, ways, part_rows, *refs),
        out_shape=jax.ShapeDtypeStruct(out_shape, F32),
        in_specs=[vmem, vmem],
        out_specs=hbm,
        scratch_shapes=[
            pltpu.VMEM((streams, FIRST, LANES), F32),
            pltpu.VMEM(out_shape, F32),
            dma((streams, own // part_rows)),
        ],
        compiler_params=pltpu.CompilerParams(vmem_limit_bytes=24 << 20),
        name="equalize",
    )(got, scales)


def solution(mesh):
    in_specs = (P("stream", None, "tm"), P())
    out_specs = P("stream", None, "tm", None)
    return jax.shard_map(shards, mesh=mesh, in_specs=in_specs, out_specs=out_specs, check_vma=False)
```

```python
import math

import jax
import jax.numpy as jnp
import numpy as np
from jax import lax
from jax.experimental import pallas as pl
from jax.experimental.pallas import tpu as pltpu
from jax.sharding import PartitionSpec as P

MESH = pl.DeviceIdType.MESH
F32 = jnp.float32
BF16 = jnp.bfloat16

LANES = 128
FIRST = 32
GROUP = 8
TAPS_PITCH = 72
FRAME_PITCH = 72
UNROLL = 4
PART_ROWS = 2
SPAN = 125.0
PEERS = ((2, 1), (2, 0), (1, 1), (3, 1), (0, 1), (1, 0), (3, 0))


def constant_table():
    index = np.arange(LANES)
    angle = 2.0 * math.pi * (np.outer(index, index) % LANES) / LANES
    cos, sin = np.cos(angle) / 64.0, np.sin(angle) / 64.0
    matrix = np.block([[cos, sin], [-sin, cos]])
    high = matrix.astype(jnp.bfloat16).astype(np.float64)
    twist = 2.0 * math.pi * np.outer(np.arange(FIRST), index) / (FIRST * LANES)
    return np.concatenate([high, matrix - high, np.concatenate([np.cos(twist), np.sin(twist)], axis=1)]).astype(np.float32)


def plus(a, b):
    return a[0] + b[0], a[1] + b[1]


def minus(a, b):
    return a[0] - b[0], a[1] - b[1]


def minus_i(a):
    return a[1], -a[0]


def turned(a, step, points):
    step %= points
    if step == 0:
        return a
    if step * 4 == points:
        return a[1], -a[0]
    if step * 2 == points:
        return -a[0], -a[1]
    if step * 8 == points:
        c = np.float32(math.sqrt(0.5))
        return (a[0] + a[1]) * c, (a[1] - a[0]) * c
    if step * 8 == 3 * points:
        c = np.float32(math.sqrt(0.5))
        return (a[1] - a[0]) * c, (a[0] + a[1]) * -c
    c = np.float32(math.cos(2.0 * math.pi * step / points))
    s = np.float32(math.sin(2.0 * math.pi * step / points))
    return a[0] * c + a[1] * s, a[1] * c - a[0] * s


def four(v):
    a, b = plus(v[0], v[2]), minus(v[0], v[2])
    c, d = plus(v[1], v[3]), minus_i(minus(v[1], v[3]))
    return [plus(a, c), plus(b, d), minus(a, c), minus(b, d)]


def eight(v):
    even, odd = four(v[0::2]), four(v[1::2])
    odd = [turned(odd[i], i, 8) for i in range(4)]
    return [plus(even[i], odd[i]) for i in range(4)] + [minus(even[i], odd[i]) for i in range(4)]


def first_section(load):
    parts = [[None] * 8 for _ in range(4)]
    for b in range(8):
        column = four([load(8 * a + b) for a in range(4)])
        for p in range(4):
            parts[p][b] = turned(column[p], b * p, FIRST)
    out = [None] * FIRST
    for p in range(4):
        for q, value in enumerate(eight(parts[p])):
            out[p + 4 * q] = value
    return out


def transposed_dot(a, b):
    return lax.dot_general(a, b, (((1,), (1,)), ((), ())), preferred_element_type=F32)


def channelize(streams, frames, ways, z_ref, taps_in, constants_in, got_ref, scales_ref,
               taps_ref, constants_ref, matrix_ref, x_ref, taps_scr, frame_scr, grid_scr, channel_scr, send_ref, table_scr, table_ref,
               table_load, load_sem, halo_send, halo_recv, send_sem, recv_sem, table_send, table_recv, own_sem, own_table_sem):
    rows = 2 * FIRST
    halo = 16 * rows
    edge = 15 * rows
    own = LANES // ways
    me = lax.axis_index("tm")
    across, along = me // 2, lax.rem(me, 2)

    def peer_of(number):
        dx, dy = PEERS[number]
        return lax.rem(across + dx, ways // 2) * 2 + lax.rem(along + dy, 2)

    barrier = pltpu.get_barrier_semaphore()
    for number in range(ways - 1):
        pl.semaphore_signal(barrier, inc=1, device_id={"tm": peer_of(number)}, device_id_type=MESH)

    def load(s):
        return pltpu.make_async_copy(z_ref.at[s], x_ref.at[s, pl.ds(halo, frames * rows), :], load_sem.at[s])

    def pass_on(s):
        return pltpu.make_async_remote_copy(
            src_ref=z_ref.at[s, pl.ds(frames * rows - edge, edge), :],
            dst_ref=x_ref.at[s, pl.ds(halo - edge, edge), :],
            send_sem=halo_send.at[s],
            recv_sem=halo_recv.at[s],
            device_id={"tm": lax.rem(me + 1, ways)},
            device_id_type=MESH,
        )

    tables = [
        pltpu.make_async_copy(taps_in, taps_ref, table_load.at[0]),
        pltpu.make_async_copy(constants_in, constants_ref, table_load.at[1]),
    ]
    tables[0].start()
    for s in range(streams):
        load(s).start()
    tables[1].start()
    @pl.when(me == 0)
    def _():
        for s in range(streams):
            x_ref[s, pl.ds(halo - edge, edge), :] = jnp.zeros((edge, LANES), BF16)

    pl.semaphore_wait(barrier, ways - 1)

    @pl.when(me < ways - 1)
    def _():
        for s in range(streams):
            pass_on(s).start()

    for copy in tables:
        copy.wait()
    for row in range(0, 4 * LANES, 64):
        matrix_ref[row : row + 64, :] = constants_ref[row : row + 64, :].astype(BF16)
    for octet in range(2):
        for m1 in range(FIRST):
            block = taps_ref[pl.ds(8 * octet, 8), pl.ds(LANES * m1, LANES)]
            for part in range(2):
                taps_scr[pl.ds(8 * octet * TAPS_PITCH + 2 * m1 + part, 8, stride=TAPS_PITCH), :] = block

    lane = lax.broadcasted_iota(jnp.int32, (LANES, LANES), 1)
    lane_c1 = lax.bitwise_and(lane, FIRST - 1)

    def transform(s, tb):
        for g in range(rows // 16):
            total = [None] * 8
            for j in range(23):
                start = pl.multiple_of((8 * tb + 1 + j) * rows + 16 * g, 16)
                x = x_ref[s, pl.ds(start, 16), :].astype(F32)
                for o in range(8):
                    k = o + 15 - j
                    if 0 <= k < 16:
                        term = taps_scr[k * TAPS_PITCH + 16 * g : k * TAPS_PITCH + 16 * g + 16, :] * x
                        total[o] = term if total[o] is None else total[o] + term
            for o in range(8):
                frame_scr[o * FRAME_PITCH + 16 * g : o * FRAME_PITCH + 16 * g + 16, :] = total[o]

        def fetch(m1):
            return tuple(frame_scr[pl.ds(2 * m1 + part, 8, stride=FRAME_PITCH), :] for part in range(2))

        at = pl.ds(pl.multiple_of(8 * tb, 8), 8)
        for c1, (real, imag) in enumerate(first_section(fetch)):
            cos, sin = (constants_ref[4 * LANES + c1 : 4 * LANES + c1 + 1, k * LANES : (k + 1) * LANES] for k in range(2))
            grid_scr[c1, at, 0:LANES] = real * cos + imag * sin
            grid_scr[c1, at, LANES : 2 * LANES] = imag * cos - real * sin

    def outgoing(s, h, number):
        peer = peer_of(number)
        return pltpu.make_async_remote_copy(
            src_ref=send_ref.at[s, h, peer],
            dst_ref=got_ref.at[s, h, me],
            send_sem=send_sem.at[s, h, number],
            recv_sem=recv_sem.at[s, h, me],
            device_id={"tm": peer},
            device_id_type=MESH,
        )

    def outgoing_table(s, number):
        peer = peer_of(number)
        return pltpu.make_async_remote_copy(
            src_ref=table_ref.at[s, pl.ds(pl.multiple_of(peer * own, own), own), :],
            dst_ref=scales_ref.at[s, me],
            send_sem=table_send.at[s, number],
            recv_sem=table_recv.at[s, me],
            device_id={"tm": peer},
            device_id_type=MESH,
        )

    def own_block(s, h):
        return pltpu.make_async_copy(send_ref.at[s, h, me], got_ref.at[s, h, me], own_sem.at[s, h])

    def own_table(s):
        return pltpu.make_async_copy(
            table_ref.at[s, pl.ds(pl.multiple_of(me * own, own), own), :], scales_ref.at[s, me], own_table_sem.at[s]
        )

    def incoming(s, h, number):
        peer = peer_of(number)
        return pltpu.make_async_remote_copy(
            src_ref=send_ref.at[s, h, peer],
            dst_ref=got_ref.at[s, h, peer],
            send_sem=send_sem.at[s, h, number],
            recv_sem=recv_sem.at[s, h, peer],
            device_id={"tm": peer},
            device_id_type=MESH,
        )

    def incoming_table(s, number):
        peer = peer_of(number)
        return pltpu.make_async_remote_copy(
            src_ref=table_ref.at[s, pl.ds(pl.multiple_of(peer * own, own), own), :],
            dst_ref=scales_ref.at[s, peer],
            send_sem=table_send.at[s, number],
            recv_sem=table_recv.at[s, peer],
            device_id={"tm": peer},
            device_id_type=MESH,
        )

    def second_section(h, place):
        c1 = h * GROUP + place
        y = grid_scr[c1]
        high = y.astype(BF16)
        low = (y - high.astype(F32)).astype(BF16)
        wide = transposed_dot(matrix_ref[: 2 * LANES], jnp.concatenate([high, low], axis=0))
        value = wide[:, :LANES] + wide[:, LANES:] + transposed_dot(matrix_ref[2 * LANES :], high)
        real, imag = value[:LANES], value[LANES:]
        power = jnp.sum(real * real + imag * imag, axis=1, keepdims=True)
        largest = jnp.max(jnp.maximum(jnp.abs(real), jnp.abs(imag)), axis=1, keepdims=True)
        largest = (largest * np.float32(1.0 + 2.0**-7)).astype(BF16).astype(F32)
        largest = jnp.maximum(largest, np.float32(2.0**-96))
        power_high = power.astype(BF16).astype(F32)
        mine = jnp.where(lane < FIRST, largest, jnp.where(lane < 2 * FIRST, power_high, power - power_high))
        table_scr[...] = jnp.where(lane_c1 == c1, mine, table_scr[...])
        scale = SPAN / largest
        for part, piece in enumerate((real, imag)):
            coded = jnp.exp2(piece * scale)
            for c in range(0, LANES, 8):
                channel_scr[part, pl.ds(c * GROUP + place, 8, stride=GROUP), :] = coded[c : c + 8]

    def pack(s, h, d):
        for part in range(2):
            for row in range(0, own * GROUP, 16):
                start = pl.multiple_of(d * own * GROUP + row, 16)
                send_ref[s, h, d, part, row : row + 16, :] = channel_scr[part, pl.ds(start, 16), :].astype(BF16)

    blocks = frames // 8

    def one_stream(s, carry):
        load(s).wait()
        lax.fori_loop(2, blocks, lambda tb, c: (transform(s, tb), c)[1], 0)

        @pl.when(me > 0)
        def _():
            pass_on(s).wait_recv()

        lax.fori_loop(0, 2, lambda tb, c: (transform(s, tb), c)[1], 0)
        table_scr[...] = jnp.zeros((LANES, LANES), F32)

        def one_group(h, carry):
            lax.fori_loop(0, GROUP, lambda place, c: (second_section(h, place), c)[1], 0, unroll=UNROLL)
            lax.fori_loop(0, ways, lambda d, c: (pack(s, h, d), c)[1], 0)
            for number in range(ways - 1):
                outgoing(s, h, number).start()
            own_block(s, h).start()
            return carry

        lax.fori_loop(0, FIRST // GROUP, one_group, 0)
        table_ref[s] = table_scr[...].astype(BF16)
        for number in range(ways - 1):
            outgoing_table(s, number).start()
        own_table(s).start()
        return carry

    lax.fori_loop(0, streams, one_stream, 0)

    @pl.when(me < ways - 1)
    def _():
        for s in range(streams):
            pass_on(s).wait_send()

    def finish(s, carry):
        for h in range(FIRST // GROUP):
            for number in range(ways - 1):
                outgoing(s, h, number).wait_send()
                incoming(s, h, number).wait_recv()
            own_block(s, h).wait()
        for number in range(ways - 1):
            outgoing_table(s, number).wait_send()
            incoming_table(s, number).wait_recv()
        own_table(s).wait()
        return carry

    lax.fori_loop(0, streams, finish, 0)


def equalize(streams, frames, ways, part_rows, got_ref, scales_ref, out_ref, factor_scr, out_scr, sem):
    own = LANES // ways
    parts = own // part_rows
    for s in range(streams):
        table = scales_ref[s].reshape(ways * own, LANES).astype(F32).T
        largest, power = table[:FIRST], table[FIRST : 2 * FIRST] + table[2 * FIRST : 3 * FIRST]
        step = LANES // 2
        while step >= own:
            power = power + pltpu.roll(power, step, 1)
            step //= 2
        mean = power * np.float32(1.0 / (frames * ways))
        factor_scr[s] = largest * np.float32(math.log2(math.e) / SPAN) * lax.rsqrt(mean + 1.0)

    def copy_out(s, n):
        rows = pl.ds(n * part_rows * FIRST, part_rows * FIRST)
        return pltpu.make_async_copy(out_scr.at[s, :, rows, :], out_ref.at[s, :, rows, :], sem.at[s, n])

    def one_stream(s, carry):
        factors = factor_scr[s]
        for n in range(parts):
            for way in range(ways):
                for h in range(FIRST // GROUP):
                    for j in range(n * part_rows, (n + 1) * part_rows, 2):
                        factor = [
                            factors[h * GROUP : (h + 1) * GROUP, way * own + i : way * own + i + 1] for i in (j, j + 1)
                        ]
                        for part in range(2):
                            value = jnp.log(got_ref[s, h, way, part, j * GROUP : (j + 2) * GROUP, :].astype(F32))
                            for i in range(2):
                                row = (j + i) * FIRST + h * GROUP
                                piece = value[i * GROUP : (i + 1) * GROUP] * factor[i]
                                out_scr[s, part, row : row + GROUP, way * LANES : (way + 1) * LANES] = piece
            copy_out(s, n).start()
        return carry

    lax.fori_loop(0, streams, one_stream, 0)
    for s in range(streams):
        for n in range(parts):
            copy_out(s, n).wait()


def shards(signal, taps):
    streams, _, samples = signal.shape
    channels = taps.shape[1]
    ways = lax.axis_size("tm")
    frames = samples // channels
    rows = 2 * FIRST
    own = LANES // ways
    z = signal.reshape(streams, 2, samples // LANES, LANES).transpose(0, 2, 1, 3).reshape(streams, frames * rows, LANES)
    constants = constant_table()
    vmem = pl.BlockSpec(memory_space=pltpu.VMEM)
    hbm = pl.BlockSpec(memory_space=pltpu.HBM)
    stay = pltpu.with_memory_space_constraint
    groups = FIRST // GROUP
    dma = pltpu.SemaphoreType.DMA
    got, scales = pl.pallas_call(
        lambda *refs: channelize(streams, frames, ways, *refs),
        out_shape=(
            jax.ShapeDtypeStruct((streams, groups, ways, 2, own * GROUP, LANES), BF16),
            jax.ShapeDtypeStruct((streams, ways, own, LANES), BF16),
        ),
        in_specs=[hbm] * 3,
        out_specs=(vmem, vmem),
        scratch_shapes=[
            pltpu.VMEM(taps.shape, F32),
            pltpu.VMEM(constants.shape, F32),
            pltpu.VMEM((4 * LANES, 2 * LANES), BF16),
            pltpu.VMEM((streams, (frames + 16) * rows, LANES), BF16),
            pltpu.VMEM((16 * TAPS_PITCH, LANES), F32),
            pltpu.VMEM((8 * FRAME_PITCH, LANES), F32),
            pltpu.VMEM((FIRST, frames, 2 * LANES), F32),
            pltpu.VMEM((2, LANES * GROUP, LANES), F32),
            pltpu.VMEM((streams, groups, ways, 2, own * GROUP, LANES), BF16),
            pltpu.VMEM((LANES, LANES), F32),
            pltpu.VMEM((streams, LANES, LANES), BF16),
            dma((2,)),
            dma((streams,)),
            dma((streams,)),
            dma((streams,)),
            dma((streams, groups, ways)),
            dma((streams, groups, ways)),
            dma((streams, ways)),
            dma((streams, ways)),
            dma((streams, groups)),
            dma((streams,)),
        ],
        compiler_params=pltpu.CompilerParams(collective_id=0, has_side_effects=True, vmem_limit_bytes=48 << 20),
        name="channelize",
    )(z, stay(taps, pltpu.HBM), stay(jnp.asarray(constants), pltpu.HBM))
    part_rows = PART_ROWS
    out_shape = (streams, 2, channels // ways, frames * ways)
    return pl.pallas_call(
        lambda *refs: equalize(streams, frames, ways, part_rows, *refs),
        out_shape=jax.ShapeDtypeStruct(out_shape, F32),
        in_specs=[vmem, vmem],
        out_specs=hbm,
        scratch_shapes=[
            pltpu.VMEM((streams, FIRST, LANES), F32),
            pltpu.VMEM(out_shape, F32),
            dma((streams, own // part_rows)),
        ],
        compiler_params=pltpu.CompilerParams(vmem_limit_bytes=24 << 20),
        name="equalize",
    )(got, scales)


def solution(mesh):
    in_specs = (P("stream", None, "tm"), P())
    out_specs = P("stream", None, "tm", None)
    return jax.shard_map(shards, mesh=mesh, in_specs=in_specs, out_specs=out_specs, check_vma=False)
```

```python
import math

import jax
import jax.numpy as jnp
import numpy as np
from jax import lax
from jax.experimental import pallas as pl
from jax.experimental.pallas import tpu as pltpu
from jax.sharding import PartitionSpec as P

MESH = pl.DeviceIdType.MESH
F32 = jnp.float32
BF16 = jnp.bfloat16

LANES = 128
FIRST = 32
GROUP = 16
TAPS_PITCH = 72
FRAME_PITCH = 72
UNROLL = 4
PART_ROWS = 2
SPAN = 125.0
POWER_SPAN = SPAN / 4.5
POWER_MID = 4.0
LOG2_E = math.log2(math.e)
PEERS = ((2, 1), (2, 0), (1, 1), (3, 1), (0, 1), (1, 0), (3, 0))


def constant_table():
    index = np.arange(LANES)
    angle = 2.0 * math.pi * (np.outer(index, index) % LANES) / LANES
    cos, sin = np.cos(angle) / 64.0, np.sin(angle) / 64.0
    matrix = np.block([[cos, sin], [-sin, cos]])
    high = matrix.astype(jnp.bfloat16).astype(np.float64)
    twist = 2.0 * math.pi * np.outer(np.arange(FIRST), index) / (FIRST * LANES)
    return np.concatenate([high, matrix - high, np.concatenate([np.cos(twist), np.sin(twist)], axis=1)]).astype(np.float32)


def plus(a, b):
    return a[0] + b[0], a[1] + b[1]


def minus(a, b):
    return a[0] - b[0], a[1] - b[1]


def minus_i(a):
    return a[1], -a[0]


def turned(a, step, points):
    step %= points
    if step == 0:
        return a
    if step * 4 == points:
        return a[1], -a[0]
    if step * 2 == points:
        return -a[0], -a[1]
    if step * 8 == points:
        c = np.float32(math.sqrt(0.5))
        return (a[0] + a[1]) * c, (a[1] - a[0]) * c
    if step * 8 == 3 * points:
        c = np.float32(math.sqrt(0.5))
        return (a[1] - a[0]) * c, (a[0] + a[1]) * -c
    c = np.float32(math.cos(2.0 * math.pi * step / points))
    s = np.float32(math.sin(2.0 * math.pi * step / points))
    return a[0] * c + a[1] * s, a[1] * c - a[0] * s


def four(v):
    a, b = plus(v[0], v[2]), minus(v[0], v[2])
    c, d = plus(v[1], v[3]), minus_i(minus(v[1], v[3]))
    return [plus(a, c), plus(b, d), minus(a, c), minus(b, d)]


def eight(v):
    even, odd = four(v[0::2]), four(v[1::2])
    odd = [turned(odd[i], i, 8) for i in range(4)]
    return [plus(even[i], odd[i]) for i in range(4)] + [minus(even[i], odd[i]) for i in range(4)]


def first_section(load):
    parts = [[None] * 8 for _ in range(4)]
    for b in range(8):
        column = four([load(8 * a + b) for a in range(4)])
        for p in range(4):
            parts[p][b] = turned(column[p], b * p, FIRST)
    out = [None] * FIRST
    for p in range(4):
        for q, value in enumerate(eight(parts[p])):
            out[p + 4 * q] = value
    return out


def transposed_dot(a, b):
    return lax.dot_general(a, b, (((1,), (1,)), ((), ())), preferred_element_type=F32)


def channelize(streams, frames, ways, z_ref, taps_in, constants_in, got_ref, scales_ref, early_ref,
               taps_ref, constants_ref, matrix_ref, x_ref, taps_scr, frame_scr, grid_scr, channel_scr, send_ref, table_scr, table_ref,
               table_load, load_sem, halo_send, halo_recv, send_sem, recv_sem, table_send, table_recv, own_sem, own_table_sem):
    rows = 2 * FIRST
    halo = 16 * rows
    edge = 15 * rows
    own = LANES // ways
    me = lax.axis_index("tm")
    across, along = me // 2, lax.rem(me, 2)

    def peer_of(number):
        dx, dy = PEERS[number]
        return lax.rem(across + dx, ways // 2) * 2 + lax.rem(along + dy, 2)

    barrier = pltpu.get_barrier_semaphore()
    for number in range(ways - 1):
        pl.semaphore_signal(barrier, inc=1, device_id={"tm": peer_of(number)}, device_id_type=MESH)

    def load(s):
        return pltpu.make_async_copy(z_ref.at[s], x_ref.at[s, pl.ds(halo, frames * rows), :], load_sem.at[s])

    def pass_on(s):
        return pltpu.make_async_remote_copy(
            src_ref=z_ref.at[s, pl.ds(frames * rows - edge, edge), :],
            dst_ref=x_ref.at[s, pl.ds(halo - edge, edge), :],
            send_sem=halo_send.at[s],
            recv_sem=halo_recv.at[s],
            device_id={"tm": lax.rem(me + 1, ways)},
            device_id_type=MESH,
        )

    tables = [
        pltpu.make_async_copy(taps_in, taps_ref, table_load.at[0]),
        pltpu.make_async_copy(constants_in, constants_ref, table_load.at[1]),
    ]
    tables[0].start()
    for s in range(streams):
        load(s).start()
    tables[1].start()
    @pl.when(me == 0)
    def _():
        for s in range(streams):
            x_ref[s, pl.ds(halo - edge, edge), :] = jnp.zeros((edge, LANES), BF16)

    pl.semaphore_wait(barrier, ways - 1)

    @pl.when(me < ways - 1)
    def _():
        for s in range(streams):
            pass_on(s).start()

    for copy in tables:
        copy.wait()
    for row in range(0, 4 * LANES, 64):
        matrix_ref[row : row + 64, :] = constants_ref[row : row + 64, :].astype(BF16)
    for octet in range(2):
        for m1 in range(FIRST):
            block = taps_ref[pl.ds(8 * octet, 8), pl.ds(LANES * m1, LANES)]
            for part in range(2):
                taps_scr[pl.ds(8 * octet * TAPS_PITCH + 2 * m1 + part, 8, stride=TAPS_PITCH), :] = block

    lane = lax.broadcasted_iota(jnp.int32, (LANES, LANES), 1)

    def transform(s, tb):
        for g in range(rows // 16):
            total = [None] * 8
            for j in range(23):
                start = pl.multiple_of((8 * tb + 1 + j) * rows + 16 * g, 16)
                x = x_ref[s, pl.ds(start, 16), :].astype(F32)
                for o in range(8):
                    k = o + 15 - j
                    if 0 <= k < 16:
                        term = taps_scr[k * TAPS_PITCH + 16 * g : k * TAPS_PITCH + 16 * g + 16, :] * x
                        total[o] = term if total[o] is None else total[o] + term
            for o in range(8):
                frame_scr[o * FRAME_PITCH + 16 * g : o * FRAME_PITCH + 16 * g + 16, :] = total[o]

        def fetch(m1):
            return tuple(frame_scr[pl.ds(2 * m1 + part, 8, stride=FRAME_PITCH), :] for part in range(2))

        at = pl.ds(pl.multiple_of(8 * tb, 8), 8)
        for c1, (real, imag) in enumerate(first_section(fetch)):
            cos, sin = (constants_ref[4 * LANES + c1 : 4 * LANES + c1 + 1, k * LANES : (k + 1) * LANES] for k in range(2))
            grid_scr[c1, at, 0:LANES] = real * cos + imag * sin
            grid_scr[c1, at, LANES : 2 * LANES] = imag * cos - real * sin

    def outgoing(s, h, number):
        peer = peer_of(number)
        return pltpu.make_async_remote_copy(
            src_ref=send_ref.at[s, h, peer],
            dst_ref=got_ref.at[s, h, me],
            send_sem=send_sem.at[s, h, number],
            recv_sem=recv_sem.at[s, h, me],
            device_id={"tm": peer},
            device_id_type=MESH,
        )

    def outgoing_table(number):
        peer = peer_of(number)
        return pltpu.make_async_remote_copy(
            src_ref=table_ref.at[pl.ds(pl.multiple_of(peer * own, own), own), :],
            dst_ref=scales_ref.at[me],
            send_sem=table_send.at[number],
            recv_sem=table_recv.at[me],
            device_id={"tm": peer},
            device_id_type=MESH,
        )

    def own_block(s, h):
        return pltpu.make_async_copy(send_ref.at[s, h, me], got_ref.at[s, h, me], own_sem.at[s, h])

    def own_table():
        return pltpu.make_async_copy(
            table_ref.at[pl.ds(pl.multiple_of(me * own, own), own), :], scales_ref.at[me], own_table_sem.at[0]
        )

    def incoming(s, h, number):
        peer = peer_of(number)
        return pltpu.make_async_remote_copy(
            src_ref=send_ref.at[s, h, peer],
            dst_ref=got_ref.at[s, h, peer],
            send_sem=send_sem.at[s, h, number],
            recv_sem=recv_sem.at[s, h, peer],
            device_id={"tm": peer},
            device_id_type=MESH,
        )

    def incoming_table(number):
        peer = peer_of(number)
        return pltpu.make_async_remote_copy(
            src_ref=table_ref.at[pl.ds(pl.multiple_of(peer * own, own), own), :],
            dst_ref=scales_ref.at[peer],
            send_sem=table_send.at[number],
            recv_sem=table_recv.at[peer],
            device_id={"tm": peer},
            device_id_type=MESH,
        )

    def second_section(s, h, place):
        c1 = h * GROUP + place
        y = grid_scr[c1]
        high = y.astype(BF16)
        low = (y - high.astype(F32)).astype(BF16)
        wide = transposed_dot(matrix_ref[: 2 * LANES], jnp.concatenate([high, low], axis=0))
        value = wide[:, :LANES] + wide[:, LANES:] + transposed_dot(matrix_ref[2 * LANES :], high)
        real, imag = value[:LANES], value[LANES:]
        power = jnp.sum(real * real + imag * imag, axis=1, keepdims=True)
        largest = jnp.max(jnp.maximum(jnp.abs(real), jnp.abs(imag)), axis=1, keepdims=True)
        largest = (largest * np.float32(1.0 + 2.0**-7)).astype(BF16).astype(F32)
        largest = jnp.maximum(largest, np.float32(2.0**-96))
        inverse = 1.0 / largest
        scale = inverse * SPAN
        ratio = jnp.log(power * inverse * inverse) * np.float32(POWER_SPAN * LOG2_E) - np.float32(POWER_SPAN * POWER_MID)
        place_in_table = 2 * FIRST * s + c1
        table = jnp.where(lane == place_in_table, largest, table_scr[...])
        table_scr[...] = jnp.where(lane == place_in_table + FIRST, jnp.exp2(ratio), table)
        for part, piece in enumerate((real, imag)):
            coded = jnp.exp2(piece * scale)
            for c in range(0, LANES, 8):
                channel_scr[part, pl.ds(c * GROUP + place, 8, stride=GROUP), :] = coded[c : c + 8]

    def pack(s, h, d):
        for part in range(2):
            for row in range(0, own * GROUP, 16):
                start = pl.multiple_of(d * own * GROUP + row, 16)
                send_ref[s, h, d, part, row : row + 16, :] = channel_scr[part, pl.ds(start, 16), :].astype(BF16)

    blocks = frames // 8
    groups = FIRST // GROUP
    table_scr[...] = jnp.zeros((LANES, LANES), F32)

    def one_stream(s, carry):
        load(s).wait()
        lax.fori_loop(2, blocks, lambda tb, c: (transform(s, tb), c)[1], 0)

        @pl.when(me > 0)
        def _():
            pass_on(s).wait_recv()

        lax.fori_loop(0, 2, lambda tb, c: (transform(s, tb), c)[1], 0)

        def one_group(h, carry):
            lax.fori_loop(0, GROUP, lambda place, c: (second_section(s, h, place), c)[1], 0, unroll=UNROLL)

            @pl.when(s * groups + h == streams * groups - 1)
            def _():
                table_ref[...] = table_scr[...].astype(BF16)
                for number in range(ways - 1):
                    outgoing_table(number).start()
                own_table().start()

            lax.fori_loop(0, ways, lambda d, c: (pack(s, h, d), c)[1], 0)
            for number in range(ways - 1):
                outgoing(s, h, number).start()
            own_block(s, h).start()
            return carry

        lax.fori_loop(0, groups, one_group, 0)
        return carry

    lax.fori_loop(0, streams, one_stream, 0)

    @pl.when(me < ways - 1)
    def _():
        for s in range(streams):
            pass_on(s).wait_send()

    for number in range(ways - 1):
        outgoing_table(number).wait_send()
        incoming_table(number).wait_recv()
    own_table().wait()
    for s in range(streams):
        for h in range(FIRST // GROUP):
            for number in range(ways - 1):
                outgoing(s, h, number).wait_send()
                incoming(s, h, number).wait_recv()
            own_block(s, h).wait()
        if s < streams - 1:
            factors = factors_of(frames, scales_ref[...], s)

            def decode_part(n, factors, s=s):
                for j in range(0, PART_ROWS, 2):
                    decode_rows(ways, got_ref.at[s], early_ref.at[s], n * PART_ROWS + j, j, factors)
                return pltpu.roll(factors, LANES - PART_ROWS, 1)

            lax.fori_loop(0, own // PART_ROWS, decode_part, factors)


def factors_of(frames, scales, s):
    ways, own, _ = scales.shape
    table = scales.reshape(ways * own, LANES).astype(F32).T
    largest, ratio = table[2 * FIRST * s : 2 * FIRST * s + FIRST], table[2 * FIRST * s + FIRST : 2 * FIRST * (s + 1)]
    ratio = jnp.exp2(jnp.log(ratio) * np.float32(LOG2_E / POWER_SPAN) + np.float32(POWER_MID))
    power = largest * largest * ratio
    step = LANES // 2
    while step >= own:
        power = power + pltpu.roll(power, step, 1)
        step //= 2
    mean = power * np.float32(1.0 / (frames * ways))
    return largest * np.float32(LOG2_E / SPAN) * lax.rsqrt(mean + 1.0)


def decode_rows(ways, got, out, first, column, factors):
    own = LANES // ways
    for way in range(ways):
        for h in range(FIRST // GROUP):
            for part in range(2):
                start = first * GROUP
                start = start if isinstance(start, int) else pl.multiple_of(start, 2 * GROUP)
                value = jnp.log(got[h, way, part, pl.ds(start, 2 * GROUP), :].astype(F32))
                for i in range(2):
                    at = way * own + column + i
                    row = (first + i) * FIRST + h * GROUP
                    row = row if isinstance(row, int) else pl.multiple_of(row, GROUP)
                    piece = value[i * GROUP : (i + 1) * GROUP] * factors[h * GROUP : (h + 1) * GROUP, at : at + 1]
                    out[part, pl.ds(row, GROUP), way * LANES : (way + 1) * LANES] = piece


def equalize(streams, frames, ways, got_ref, scales_ref, early_ref, out_ref, late_ref, sem):
    own = LANES // ways
    last = streams - 1
    size = PART_ROWS * FIRST

    def copy_out(s, n):
        source = early_ref.at[s] if s < last else late_ref
        rows = pl.ds(n * size, size)
        return pltpu.make_async_copy(source.at[:, rows, :], out_ref.at[s, :, rows, :], sem.at[s, n])

    parts = own // PART_ROWS
    for s in range(last):
        for n in range(parts):
            copy_out(s, n).start()
    factors = factors_of(frames, scales_ref[...], last)
    for n in range(parts):
        for j in range(n * PART_ROWS, (n + 1) * PART_ROWS, 2):
            decode_rows(ways, got_ref.at[last], late_ref, j, j, factors)
        copy_out(last, n).start()
    for s in range(streams):
        for n in range(parts):
            copy_out(s, n).wait()


def shards(signal, taps):
    streams, _, samples = signal.shape
    channels = taps.shape[1]
    ways = lax.axis_size("tm")
    frames = samples // channels
    rows = 2 * FIRST
    own = LANES // ways
    z = signal.reshape(streams, 2, samples // LANES, LANES).transpose(0, 2, 1, 3).reshape(streams, frames * rows, LANES)
    constants = constant_table()
    vmem = pl.BlockSpec(memory_space=pltpu.VMEM)
    hbm = pl.BlockSpec(memory_space=pltpu.HBM)
    stay = pltpu.with_memory_space_constraint
    groups = FIRST // GROUP
    dma = pltpu.SemaphoreType.DMA
    share = channels // ways
    got, scales, early = pl.pallas_call(
        lambda *refs: channelize(streams, frames, ways, *refs),
        out_shape=(
            jax.ShapeDtypeStruct((streams, groups, ways, 2, own * GROUP, LANES), BF16),
            jax.ShapeDtypeStruct((ways, own, LANES), BF16),
            jax.ShapeDtypeStruct((streams - 1, 2, share, frames * ways), F32),
        ),
        in_specs=[hbm] * 3,
        out_specs=(vmem, vmem, vmem),
        scratch_shapes=[
            pltpu.VMEM(taps.shape, F32),
            pltpu.VMEM(constants.shape, F32),
            pltpu.VMEM((4 * LANES, 2 * LANES), BF16),
            pltpu.VMEM((streams, (frames + 16) * rows, LANES), BF16),
            pltpu.VMEM((16 * TAPS_PITCH, LANES), F32),
            pltpu.VMEM((8 * FRAME_PITCH, LANES), F32),
            pltpu.VMEM((FIRST, frames, 2 * LANES), F32),
            pltpu.VMEM((2, LANES * GROUP, LANES), F32),
            pltpu.VMEM((streams, groups, ways, 2, own * GROUP, LANES), BF16),
            pltpu.VMEM((LANES, LANES), F32),
            pltpu.VMEM((LANES, LANES), BF16),
            dma((2,)),
            dma((streams,)),
            dma((streams,)),
            dma((streams,)),
            dma((streams, groups, ways)),
            dma((streams, groups, ways)),
            dma((ways,)),
            dma((ways,)),
            dma((streams, groups)),
            dma((1,)),
        ],
        compiler_params=pltpu.CompilerParams(collective_id=0, has_side_effects=True, vmem_limit_bytes=40 << 20),
        name="channelize",
    )(stay(z, pltpu.HBM), stay(taps, pltpu.HBM), stay(jnp.asarray(constants), pltpu.HBM))
    return pl.pallas_call(
        lambda *refs: equalize(streams, frames, ways, *refs),
        out_shape=jax.ShapeDtypeStruct((streams, 2, share, frames * ways), F32),
        in_specs=[vmem, vmem, vmem],
        out_specs=hbm,
        scratch_shapes=[pltpu.VMEM((2, share, frames * ways), F32), dma((streams, own // PART_ROWS))],
        compiler_params=pltpu.CompilerParams(vmem_limit_bytes=24 << 20),
        name="equalize",
    )(got, scales, early)


def solution(mesh):
    in_specs = (P("stream", None, "tm"), P())
    out_specs = P("stream", None, "tm", None)
    return jax.shard_map(shards, mesh=mesh, in_specs=in_specs, out_specs=out_specs, check_vma=False)
```

```python
import math

import jax
import jax.numpy as jnp
import numpy as np
from jax import lax
from jax.experimental import pallas as pl
from jax.experimental.pallas import tpu as pltpu
from jax.sharding import PartitionSpec as P

MESH = pl.DeviceIdType.MESH
F32 = jnp.float32
BF16 = jnp.bfloat16

LANES = 128
FIRST = 32
GROUP = 16
TAPS_PITCH = 72
FRAME_PITCH = 72
UNROLL = 8
PART_ROWS = 4
SPAN = 125.0
POWER_SPAN = SPAN / 4.5
POWER_MID = 4.0
LOG2_E = math.log2(math.e)
PEERS = ((2, 1), (2, 0), (1, 1), (3, 1), (0, 1), (1, 0), (3, 0))


def constant_table():
    index = np.arange(LANES)
    angle = 2.0 * math.pi * (np.outer(index, index) % LANES) / LANES
    cos, sin = np.cos(angle) / 64.0, np.sin(angle) / 64.0
    matrix = np.block([[cos, sin], [-sin, cos]])
    high = matrix.astype(jnp.bfloat16).astype(np.float64)
    twist = 2.0 * math.pi * np.outer(np.arange(FIRST), index) / (FIRST * LANES)
    return np.concatenate([high, matrix - high, np.concatenate([np.cos(twist), np.sin(twist)], axis=1)]).astype(np.float32)


def plus(a, b):
    return a[0] + b[0], a[1] + b[1]


def minus(a, b):
    return a[0] - b[0], a[1] - b[1]


def minus_i(a):
    return a[1], -a[0]


def turned(a, step, points):
    step %= points
    if step == 0:
        return a
    if step * 4 == points:
        return a[1], -a[0]
    if step * 2 == points:
        return -a[0], -a[1]
    if step * 8 == points:
        c = np.float32(math.sqrt(0.5))
        return (a[0] + a[1]) * c, (a[1] - a[0]) * c
    if step * 8 == 3 * points:
        c = np.float32(math.sqrt(0.5))
        return (a[1] - a[0]) * c, (a[0] + a[1]) * -c
    c = np.float32(math.cos(2.0 * math.pi * step / points))
    s = np.float32(math.sin(2.0 * math.pi * step / points))
    return a[0] * c + a[1] * s, a[1] * c - a[0] * s


def four(v):
    a, b = plus(v[0], v[2]), minus(v[0], v[2])
    c, d = plus(v[1], v[3]), minus_i(minus(v[1], v[3]))
    return [plus(a, c), plus(b, d), minus(a, c), minus(b, d)]


def eight(v):
    even, odd = four(v[0::2]), four(v[1::2])
    odd = [turned(odd[i], i, 8) for i in range(4)]
    return [plus(even[i], odd[i]) for i in range(4)] + [minus(even[i], odd[i]) for i in range(4)]


def first_section(load):
    parts = [[None] * 8 for _ in range(4)]
    for b in range(8):
        column = four([load(8 * a + b) for a in range(4)])
        for p in range(4):
            parts[p][b] = turned(column[p], b * p, FIRST)
    out = [None] * FIRST
    for p in range(4):
        for q, value in enumerate(eight(parts[p])):
            out[p + 4 * q] = value
    return out


def transposed_dot(a, b):
    return lax.dot_general(a, b, (((1,), (1,)), ((), ())), preferred_element_type=F32)


def channelize(streams, frames, ways, z_ref, taps_in, constants_in, got_ref, factors_ref, early_ref, late_ref,
               scales_ref, taps_ref, constants_ref, matrix_ref, x_ref, taps_scr, frame_scr, grid_scr, channel_scr, send_ref, table_scr, table_ref,
               table_load, load_sem, halo_send, halo_recv, send_sem, recv_sem, table_send, table_recv, own_sem, own_table_sem):
    rows = 2 * FIRST
    halo = 16 * rows
    edge = 15 * rows
    own = LANES // ways
    me = lax.axis_index("tm")
    across, along = me // 2, lax.rem(me, 2)

    def peer_of(number):
        dx, dy = PEERS[number]
        return lax.rem(across + dx, ways // 2) * 2 + lax.rem(along + dy, 2)

    barrier = pltpu.get_barrier_semaphore()
    for number in range(ways - 1):
        pl.semaphore_signal(barrier, inc=1, device_id={"tm": peer_of(number)}, device_id_type=MESH)

    def load(s):
        return pltpu.make_async_copy(z_ref.at[s], x_ref.at[s, pl.ds(halo, frames * rows), :], load_sem.at[s])

    def pass_on(s):
        return pltpu.make_async_remote_copy(
            src_ref=z_ref.at[s, pl.ds(frames * rows - edge, edge), :],
            dst_ref=x_ref.at[s, pl.ds(halo - edge, edge), :],
            send_sem=halo_send.at[s],
            recv_sem=halo_recv.at[s],
            device_id={"tm": lax.rem(me + 1, ways)},
            device_id_type=MESH,
        )

    tables = [
        pltpu.make_async_copy(taps_in, taps_ref, table_load.at[0]),
        pltpu.make_async_copy(constants_in, constants_ref, table_load.at[1]),
    ]
    tables[0].start()
    for s in range(streams):
        load(s).start()
    tables[1].start()
    @pl.when(me == 0)
    def _():
        for s in range(streams):
            x_ref[s, pl.ds(halo - edge, edge), :] = jnp.zeros((edge, LANES), BF16)

    pl.semaphore_wait(barrier, ways - 1)

    @pl.when(me < ways - 1)
    def _():
        for s in range(streams):
            pass_on(s).start()

    for copy in tables:
        copy.wait()
    for row in range(0, 4 * LANES, 64):
        matrix_ref[row : row + 64, :] = constants_ref[row : row + 64, :].astype(BF16)
    for octet in range(2):
        for m1 in range(FIRST):
            block = taps_ref[pl.ds(8 * octet, 8), pl.ds(LANES * m1, LANES)]
            for part in range(2):
                taps_scr[pl.ds(8 * octet * TAPS_PITCH + 2 * m1 + part, 8, stride=TAPS_PITCH), :] = block

    lane = lax.broadcasted_iota(jnp.int32, (LANES, LANES), 1)

    def transform(s, tb):
        for g in range(rows // 16):
            total = [None] * 8
            for j in range(23):
                start = pl.multiple_of((8 * tb + 1 + j) * rows + 16 * g, 16)
                x = x_ref[s, pl.ds(start, 16), :].astype(F32)
                for o in range(8):
                    k = o + 15 - j
                    if 0 <= k < 16:
                        term = taps_scr[k * TAPS_PITCH + 16 * g : k * TAPS_PITCH + 16 * g + 16, :] * x
                        total[o] = term if total[o] is None else total[o] + term
            for o in range(8):
                frame_scr[o * FRAME_PITCH + 16 * g : o * FRAME_PITCH + 16 * g + 16, :] = total[o]

        def fetch(m1):
            return tuple(frame_scr[pl.ds(2 * m1 + part, 8, stride=FRAME_PITCH), :] for part in range(2))

        at = pl.ds(pl.multiple_of(8 * tb, 8), 8)
        for c1, (real, imag) in enumerate(first_section(fetch)):
            cos, sin = (constants_ref[4 * LANES + c1 : 4 * LANES + c1 + 1, k * LANES : (k + 1) * LANES] for k in range(2))
            grid_scr[c1, at, 0:LANES] = real * cos + imag * sin
            grid_scr[c1, at, LANES : 2 * LANES] = imag * cos - real * sin

    def outgoing(s, h, number):
        peer = peer_of(number)
        return pltpu.make_async_remote_copy(
            src_ref=send_ref.at[s, h, peer],
            dst_ref=got_ref.at[s, h, me],
            send_sem=send_sem.at[s, h, number],
            recv_sem=recv_sem.at[s, h, me],
            device_id={"tm": peer},
            device_id_type=MESH,
        )

    def outgoing_table(number):
        peer = peer_of(number)
        return pltpu.make_async_remote_copy(
            src_ref=table_ref.at[pl.ds(pl.multiple_of(peer * own, own), own), :],
            dst_ref=scales_ref.at[me],
            send_sem=table_send.at[number],
            recv_sem=table_recv.at[me],
            device_id={"tm": peer},
            device_id_type=MESH,
        )

    def own_block(s, h):
        return pltpu.make_async_copy(send_ref.at[s, h, me], got_ref.at[s, h, me], own_sem.at[s, h])

    def own_table():
        return pltpu.make_async_copy(
            table_ref.at[pl.ds(pl.multiple_of(me * own, own), own), :], scales_ref.at[me], own_table_sem.at[0]
        )

    def incoming(s, h, number):
        peer = peer_of(number)
        return pltpu.make_async_remote_copy(
            src_ref=send_ref.at[s, h, peer],
            dst_ref=got_ref.at[s, h, peer],
            send_sem=send_sem.at[s, h, number],
            recv_sem=recv_sem.at[s, h, peer],
            device_id={"tm": peer},
            device_id_type=MESH,
        )

    def incoming_table(number):
        peer = peer_of(number)
        return pltpu.make_async_remote_copy(
            src_ref=table_ref.at[pl.ds(pl.multiple_of(peer * own, own), own), :],
            dst_ref=scales_ref.at[peer],
            send_sem=table_send.at[number],
            recv_sem=table_recv.at[peer],
            device_id={"tm": peer},
            device_id_type=MESH,
        )

    def second_section(s, h, place):
        c1 = h * GROUP + place
        y = grid_scr[c1]
        high = y.astype(BF16)
        low = (y - high.astype(F32)).astype(BF16)
        wide = transposed_dot(matrix_ref[: 2 * LANES], jnp.concatenate([high, low], axis=0))
        value = wide[:, :LANES] + wide[:, LANES:] + transposed_dot(matrix_ref[2 * LANES :], high)
        real, imag = value[:LANES], value[LANES:]
        power = jnp.sum(real * real + imag * imag, axis=1, keepdims=True)
        largest = jnp.max(jnp.maximum(jnp.abs(real), jnp.abs(imag)), axis=1, keepdims=True)
        largest = (largest * np.float32(1.0 + 2.0**-7)).astype(BF16).astype(F32)
        largest = jnp.maximum(largest, np.float32(2.0**-118))
        inverse = 1.0 / largest
        scale = inverse * SPAN
        ratio = jnp.log(power * inverse * inverse) * np.float32(POWER_SPAN * LOG2_E) - np.float32(POWER_SPAN * POWER_MID)
        place_in_table = 2 * FIRST * s + c1
        table = jnp.where(lane == place_in_table, largest, table_scr[...])
        table_scr[...] = jnp.where(lane == place_in_table + FIRST, jnp.exp2(ratio), table)
        for part, piece in enumerate((real, imag)):
            coded = jnp.exp2(piece * scale)
            for c in range(0, LANES, 8):
                channel_scr[part, pl.ds(c * GROUP + place, 8, stride=GROUP), :] = coded[c : c + 8]

    def pack(s, h, d):
        for part in range(2):
            for row in range(0, own * GROUP, 16):
                start = pl.multiple_of(d * own * GROUP + row, 16)
                send_ref[s, h, d, part, row : row + 16, :] = channel_scr[part, pl.ds(start, 16), :].astype(BF16)

    blocks = frames // 8
    groups = FIRST // GROUP
    table_scr[...] = jnp.zeros((LANES, LANES), F32)

    def one_stream(s, carry):
        load(s).wait()
        lax.fori_loop(2, blocks, lambda tb, c: (transform(s, tb), c)[1], 0)

        @pl.when(me > 0)
        def _():
            pass_on(s).wait_recv()

        lax.fori_loop(0, 2, lambda tb, c: (transform(s, tb), c)[1], 0)

        def one_group(h, carry):
            lax.fori_loop(0, GROUP, lambda place, c: (second_section(s, h, place), c)[1], 0, unroll=UNROLL)

            @pl.when(s * groups + h == streams * groups - 1)
            def _():
                table_ref[...] = table_scr[...].astype(BF16)
                for number in range(ways - 1):
                    outgoing_table(number).start()
                own_table().start()

            lax.fori_loop(0, ways, lambda d, c: (pack(s, h, d), c)[1], 0)
            for number in range(ways - 1):
                outgoing(s, h, number).start()
            own_block(s, h).start()
            return carry

        lax.fori_loop(0, groups, one_group, 0)
        return carry

    lax.fori_loop(0, streams, one_stream, 0)

    @pl.when(me < ways - 1)
    def _():
        for s in range(streams):
            pass_on(s).wait_send()

    for number in range(ways - 1):
        outgoing_table(number).wait_send()
        incoming_table(number).wait_recv()
    own_table().wait()
    scales = scales_ref[...]
    factors_ref[...] = factors_of(frames, scales, streams - 1)
    for s in range(streams):
        factors = factors_of(frames, scales, s)
        for h in range(groups):
            for number in range(ways - 1):
                outgoing(s, h, number).wait_send()
                incoming(s, h, number).wait_recv()
            own_block(s, h).wait()
            if (s, h) == (streams - 1, groups - 1):
                break
            target = early_ref.at[s] if s < streams - 1 else late_ref

            def decode_part(n, factors, s=s, h=h, target=target):
                for j in range(PART_ROWS):
                    decode_row(ways, got_ref.at[s, h], target, n * PART_ROWS + j, j, h * GROUP, factors[h * GROUP : (h + 1) * GROUP])
                return pltpu.roll(factors, LANES - PART_ROWS, 1)

            lax.fori_loop(0, own // PART_ROWS, decode_part, factors)


def factors_of(frames, scales, s):
    ways, own, _ = scales.shape
    table = scales.reshape(ways * own, LANES).astype(F32).T
    largest, ratio = table[2 * FIRST * s : 2 * FIRST * s + FIRST], table[2 * FIRST * s + FIRST : 2 * FIRST * (s + 1)]
    ratio = jnp.exp2(jnp.log(ratio) * np.float32(LOG2_E / POWER_SPAN) + np.float32(POWER_MID))
    power = largest * largest * ratio
    step = LANES // 2
    while step >= own:
        power = power + pltpu.roll(power, step, 1)
        step //= 2
    mean = power * np.float32(1.0 / (frames * ways))
    return largest * np.float32(LOG2_E / SPAN) * lax.rsqrt(mean + 1.0)


def decode_row(ways, got, out, j, column, row, factors):
    own = LANES // ways
    start = j * GROUP
    start = start if isinstance(start, int) else pl.multiple_of(start, GROUP)
    for way in range(ways):
        at = way * own + column
        for part in range(2):
            value = jnp.log(got[way, part, pl.ds(start, GROUP), :].astype(F32))
            out[part, j, row : row + GROUP, way * LANES : (way + 1) * LANES] = value * factors[:, at : at + 1]


def equalize(streams, ways, got_ref, factors_ref, early_ref, late_ref, out_ref, last_ref, early_sem, late_sem, last_sem):
    own = LANES // ways
    s, h = streams - 1, FIRST // GROUP - 1

    def copy_early(n):
        return pltpu.make_async_copy(early_ref.at[n], out_ref.at[n], early_sem.at[n])

    def copy_late():
        return pltpu.make_async_copy(late_ref, out_ref.at[s, :, :, pl.ds(0, h * GROUP), :], late_sem.at[0])

    def copy_last(n):
        rows = pl.ds(n * PART_ROWS, PART_ROWS)
        return pltpu.make_async_copy(
            last_ref.at[:, rows], out_ref.at[s, :, rows, pl.ds(h * GROUP, GROUP), :], last_sem.at[n]
        )

    for n in range(s):
        copy_early(n).start()
    copy_late().start()
    factors = factors_ref[h * GROUP :, :]
    for n in range(own // PART_ROWS):
        for j in range(n * PART_ROWS, (n + 1) * PART_ROWS):
            decode_row(ways, got_ref.at[s, h], last_ref, j, j, 0, factors)
        copy_last(n).start()
    for n in range(s):
        copy_early(n).wait()
    copy_late().wait()
    for n in range(own // PART_ROWS):
        copy_last(n).wait()


def shards(signal, taps):
    streams, _, samples = signal.shape
    channels = taps.shape[1]
    ways = lax.axis_size("tm")
    frames = samples // channels
    rows = 2 * FIRST
    own = LANES // ways
    z = signal.reshape(streams, 2, samples // LANES, LANES).transpose(0, 2, 1, 3).reshape(streams, frames * rows, LANES)
    constants = constant_table()
    vmem = pl.BlockSpec(memory_space=pltpu.VMEM)
    hbm = pl.BlockSpec(memory_space=pltpu.HBM)
    stay = pltpu.with_memory_space_constraint
    groups = FIRST // GROUP
    dma = pltpu.SemaphoreType.DMA
    share = channels // ways
    got, factors, early, late = pl.pallas_call(
        lambda *refs: channelize(streams, frames, ways, *refs),
        out_shape=(
            jax.ShapeDtypeStruct((streams, groups, ways, 2, own * GROUP, LANES), BF16),
            jax.ShapeDtypeStruct((FIRST, LANES), F32),
            jax.ShapeDtypeStruct((streams - 1, 2, own, FIRST, frames * ways), F32),
            jax.ShapeDtypeStruct((2, own, FIRST - GROUP, frames * ways), F32),
        ),
        in_specs=[hbm] * 3,
        out_specs=(vmem, vmem, vmem, vmem),
        scratch_shapes=[
            pltpu.VMEM((ways, own, LANES), BF16),
            pltpu.VMEM(taps.shape, F32),
            pltpu.VMEM(constants.shape, F32),
            pltpu.VMEM((4 * LANES, 2 * LANES), BF16),
            pltpu.VMEM((streams, (frames + 16) * rows, LANES), BF16),
            pltpu.VMEM((17 * TAPS_PITCH, LANES), F32),
            pltpu.VMEM((9 * FRAME_PITCH, LANES), F32),
            pltpu.VMEM((FIRST, frames, 2 * LANES), F32),
            pltpu.VMEM((2, (LANES + 1) * GROUP, LANES), F32),
            pltpu.VMEM((streams, groups, ways, 2, own * GROUP, LANES), BF16),
            pltpu.VMEM((LANES, LANES), F32),
            pltpu.VMEM((LANES, LANES), BF16),
            dma((2,)),
            dma((streams,)),
            dma((streams,)),
            dma((streams,)),
            dma((streams, groups, ways)),
            dma((streams, groups, ways)),
            dma((ways,)),
            dma((ways,)),
            dma((streams, groups)),
            dma((1,)),
        ],
        compiler_params=pltpu.CompilerParams(collective_id=0, has_side_effects=True, vmem_limit_bytes=40 << 20),
        name="channelize",
    )(stay(z, pltpu.HBM), stay(taps, pltpu.HBM), stay(jnp.asarray(constants), pltpu.HBM))
    out = pl.pallas_call(
        lambda *refs: equalize(streams, ways, *refs),
        out_shape=jax.ShapeDtypeStruct((streams, 2, own, FIRST, frames * ways), F32),
        in_specs=[vmem, vmem, vmem, vmem],
        out_specs=hbm,
        scratch_shapes=[
            pltpu.VMEM((2, own, GROUP, frames * ways), F32),
            dma((streams - 1,)),
            dma((1,)),
            dma((own // PART_ROWS,)),
        ],
        compiler_params=pltpu.CompilerParams(vmem_limit_bytes=16 << 20),
        name="equalize",
    )(got, factors, early, late)
    return out.reshape(streams, 2, share, frames * ways)


def solution(mesh):
    in_specs = (P("stream", None, "tm"), P())
    out_specs = P("stream", None, "tm", None)
    return jax.shard_map(shards, mesh=mesh, in_specs=in_specs, out_specs=out_specs, check_vma=False)
```

```python
import math

import jax
import jax.numpy as jnp
import numpy as np
from jax import lax
from jax.experimental import pallas as pl
from jax.experimental.pallas import tpu as pltpu
from jax.sharding import PartitionSpec as P

MESH = pl.DeviceIdType.MESH
F32 = jnp.float32
BF16 = jnp.bfloat16

LANES = 128
FIRST = 32
GROUP = 16
TAPS_PITCH = 72
FRAME_PITCH = 72
UNROLL = 16
PART_ROWS = 4
SPAN = 125.0
POWER_SPAN = SPAN / 4.5
POWER_MID = 4.0
LOG2_E = math.log2(math.e)
PEERS = ((2, 1), (2, 0), (1, 1), (3, 1), (0, 1), (1, 0), (3, 0))


def constant_table():
    index = np.arange(LANES)
    angle = 2.0 * math.pi * (np.outer(index, index) % LANES) / LANES
    cos, sin = np.cos(angle) / 64.0, np.sin(angle) / 64.0
    matrix = np.block([[cos, sin], [-sin, cos]])
    high = matrix.astype(jnp.bfloat16).astype(np.float64)
    twist = 2.0 * math.pi * np.outer(np.arange(FIRST), index) / (FIRST * LANES)
    return np.concatenate([high, matrix - high, np.concatenate([np.cos(twist), np.sin(twist)], axis=1)]).astype(np.float32)


def plus(a, b):
    return a[0] + b[0], a[1] + b[1]


def minus(a, b):
    return a[0] - b[0], a[1] - b[1]


def minus_i(a):
    return a[1], -a[0]


def turned(a, step, points):
    step %= points
    if step == 0:
        return a
    if step * 4 == points:
        return a[1], -a[0]
    if step * 2 == points:
        return -a[0], -a[1]
    if step * 8 == points:
        c = np.float32(math.sqrt(0.5))
        return (a[0] + a[1]) * c, (a[1] - a[0]) * c
    if step * 8 == 3 * points:
        c = np.float32(math.sqrt(0.5))
        return (a[1] - a[0]) * c, (a[0] + a[1]) * -c
    c = np.float32(math.cos(2.0 * math.pi * step / points))
    s = np.float32(math.sin(2.0 * math.pi * step / points))
    return a[0] * c + a[1] * s, a[1] * c - a[0] * s


def four(v):
    a, b = plus(v[0], v[2]), minus(v[0], v[2])
    c, d = plus(v[1], v[3]), minus_i(minus(v[1], v[3]))
    return [plus(a, c), plus(b, d), minus(a, c), minus(b, d)]


def eight(v):
    even, odd = four(v[0::2]), four(v[1::2])
    odd = [turned(odd[i], i, 8) for i in range(4)]
    return [plus(even[i], odd[i]) for i in range(4)] + [minus(even[i], odd[i]) for i in range(4)]


def first_section(load):
    parts = [[None] * 8 for _ in range(4)]
    for b in range(8):
        column = four([load(8 * a + b) for a in range(4)])
        for p in range(4):
            parts[p][b] = turned(column[p], b * p, FIRST)
    out = [None] * FIRST
    for p in range(4):
        for q, value in enumerate(eight(parts[p])):
            out[p + 4 * q] = value
    return out


def transposed_dot(a, b):
    return lax.dot_general(a, b, (((1,), (1,)), ((), ())), preferred_element_type=F32)


def channelize(streams, frames, ways, z_ref, taps_in, constants_in, got_ref, factors_ref, early_ref, late_ref,
               scales_ref, taps_ref, constants_ref, matrix_ref, x_ref, taps_scr, frame_scr, grid_scr, channel_scr, send_ref, table_scr, table_ref,
               table_load, load_sem, halo_send, halo_recv, send_sem, recv_sem, table_send, table_recv, own_sem, own_table_sem):
    rows = 2 * FIRST
    halo = 16 * rows
    edge = 15 * rows
    own = LANES // ways
    me = lax.axis_index("tm")
    across, along = me // 2, lax.rem(me, 2)

    def peer_of(number):
        dx, dy = PEERS[number]
        return lax.rem(across + dx, ways // 2) * 2 + lax.rem(along + dy, 2)

    barrier = pltpu.get_barrier_semaphore()
    for number in range(ways - 1):
        pl.semaphore_signal(barrier, inc=1, device_id={"tm": peer_of(number)}, device_id_type=MESH)

    def load(s):
        return pltpu.make_async_copy(z_ref.at[s], x_ref.at[s, pl.ds(halo, frames * rows), :], load_sem.at[s])

    def pass_on(s):
        return pltpu.make_async_remote_copy(
            src_ref=z_ref.at[s, pl.ds(frames * rows - edge, edge), :],
            dst_ref=x_ref.at[s, pl.ds(halo - edge, edge), :],
            send_sem=halo_send.at[s],
            recv_sem=halo_recv.at[s],
            device_id={"tm": lax.rem(me + 1, ways)},
            device_id_type=MESH,
        )

    tables = [
        pltpu.make_async_copy(taps_in, taps_ref, table_load.at[0]),
        pltpu.make_async_copy(constants_in, constants_ref, table_load.at[1]),
    ]
    tables[0].start()
    for s in range(streams):
        load(s).start()
    tables[1].start()
    @pl.when(me == 0)
    def _():
        for s in range(streams):
            x_ref[s, pl.ds(halo - edge, edge), :] = jnp.zeros((edge, LANES), BF16)

    pl.semaphore_wait(barrier, ways - 1)

    @pl.when(me < ways - 1)
    def _():
        for s in range(streams):
            pass_on(s).start()

    for copy in tables:
        copy.wait()
    for row in range(0, 4 * LANES, 64):
        matrix_ref[row : row + 64, :] = constants_ref[row : row + 64, :].astype(BF16)
    for octet in range(2):
        for m1 in range(FIRST):
            block = taps_ref[pl.ds(8 * octet, 8), pl.ds(LANES * m1, LANES)]
            for part in range(2):
                taps_scr[pl.ds(8 * octet * TAPS_PITCH + 2 * m1 + part, 8, stride=TAPS_PITCH), :] = block

    lane = lax.broadcasted_iota(jnp.int32, (LANES, LANES), 1)

    def transform(s, tb, slot):
        base = slot * 9 * FRAME_PITCH
        for g in range(rows // 16):
            total = [None] * 8
            for j in range(23):
                start = pl.multiple_of((8 * tb + 1 + j) * rows + 16 * g, 16)
                x = x_ref[s, pl.ds(start, 16), :].astype(F32)
                for o in range(8):
                    k = o + 15 - j
                    if 0 <= k < 16:
                        term = taps_scr[k * TAPS_PITCH + 16 * g : k * TAPS_PITCH + 16 * g + 16, :] * x
                        total[o] = term if total[o] is None else total[o] + term
            for o in range(8):
                start = base + o * FRAME_PITCH + 16 * g
                frame_scr[start : start + 16, :] = total[o]

        def fetch(m1):
            return tuple(frame_scr[pl.ds(base + 2 * m1 + part, 8, stride=FRAME_PITCH), :] for part in range(2))

        at = pl.ds(pl.multiple_of(8 * tb, 8), 8)
        for c1, (real, imag) in enumerate(first_section(fetch)):
            cos, sin = (constants_ref[4 * LANES + c1 : 4 * LANES + c1 + 1, k * LANES : (k + 1) * LANES] for k in range(2))
            grid_scr[c1, at, 0:LANES] = real * cos + imag * sin
            grid_scr[c1, at, LANES : 2 * LANES] = imag * cos - real * sin

    def outgoing(s, h, number):
        peer = peer_of(number)
        return pltpu.make_async_remote_copy(
            src_ref=send_ref.at[s, h, peer],
            dst_ref=got_ref.at[s, h, me],
            send_sem=send_sem.at[s, h, number],
            recv_sem=recv_sem.at[s, h, me],
            device_id={"tm": peer},
            device_id_type=MESH,
        )

    def outgoing_table(number):
        peer = peer_of(number)
        return pltpu.make_async_remote_copy(
            src_ref=table_ref.at[pl.ds(pl.multiple_of(peer * own, own), own), :],
            dst_ref=scales_ref.at[me],
            send_sem=table_send.at[number],
            recv_sem=table_recv.at[me],
            device_id={"tm": peer},
            device_id_type=MESH,
        )

    def own_block(s, h):
        return pltpu.make_async_copy(send_ref.at[s, h, me], got_ref.at[s, h, me], own_sem.at[s, h])

    def own_table():
        return pltpu.make_async_copy(
            table_ref.at[pl.ds(pl.multiple_of(me * own, own), own), :], scales_ref.at[me], own_table_sem.at[0]
        )

    def incoming(s, h, number):
        peer = peer_of(number)
        return pltpu.make_async_remote_copy(
            src_ref=send_ref.at[s, h, peer],
            dst_ref=got_ref.at[s, h, peer],
            send_sem=send_sem.at[s, h, number],
            recv_sem=recv_sem.at[s, h, peer],
            device_id={"tm": peer},
            device_id_type=MESH,
        )

    def incoming_table(number):
        peer = peer_of(number)
        return pltpu.make_async_remote_copy(
            src_ref=table_ref.at[pl.ds(pl.multiple_of(peer * own, own), own), :],
            dst_ref=scales_ref.at[peer],
            send_sem=table_send.at[number],
            recv_sem=table_recv.at[peer],
            device_id={"tm": peer},
            device_id_type=MESH,
        )

    def second_section(s, h, place):
        c1 = h * GROUP + place
        y = grid_scr[c1]
        high = y.astype(BF16)
        low = (y - high.astype(F32)).astype(BF16)
        wide = transposed_dot(matrix_ref[: 2 * LANES], jnp.concatenate([high, low], axis=0))
        value = wide[:, :LANES] + wide[:, LANES:] + transposed_dot(matrix_ref[2 * LANES :], high)
        real, imag = value[:LANES], value[LANES:]
        power = jnp.sum(real * real + imag * imag, axis=1, keepdims=True)
        largest = jnp.max(jnp.maximum(jnp.abs(real), jnp.abs(imag)), axis=1, keepdims=True)
        largest = (largest * np.float32(1.0 + 2.0**-7)).astype(BF16).astype(F32)
        largest = jnp.maximum(largest, np.float32(2.0**-118))
        inverse = 1.0 / largest
        scale = inverse * SPAN
        ratio = jnp.log(power * inverse * inverse) * np.float32(POWER_SPAN * LOG2_E) - np.float32(POWER_SPAN * POWER_MID)
        place_in_table = 2 * FIRST * s + c1
        table = jnp.where(lane == place_in_table, largest, table_scr[...])
        table_scr[...] = jnp.where(lane == place_in_table + FIRST, jnp.exp2(ratio), table)
        for part, piece in enumerate((real, imag)):
            coded = jnp.exp2(piece * scale)
            for c in range(0, LANES, 8):
                channel_scr[part, pl.ds(c * GROUP + place, 8, stride=GROUP), :] = coded[c : c + 8]

    def pack(s, h, d):
        for part in range(2):
            for row in range(0, own * GROUP, 16):
                start = pl.multiple_of(d * own * GROUP + row, 16)
                send_ref[s, h, d, part, row : row + 16, :] = channel_scr[part, pl.ds(start, 16), :].astype(BF16)

    blocks = frames // 8
    groups = FIRST // GROUP
    table_scr[...] = jnp.zeros((LANES, LANES), F32)

    def one_stream(s, carry):
        load(s).wait()

        def two_blocks(pair, carry):
            for slot in range(2):
                transform(s, 2 * pair + slot, slot)
            return carry

        lax.fori_loop(1, blocks // 2, two_blocks, 0)

        @pl.when(me > 0)
        def _():
            pass_on(s).wait_recv()

        lax.fori_loop(0, 1, two_blocks, 0)

        def one_group(h, carry):
            lax.fori_loop(0, GROUP, lambda place, c: (second_section(s, h, place), c)[1], 0, unroll=UNROLL)

            @pl.when(s * groups + h == streams * groups - 1)
            def _():
                table_ref[...] = table_scr[...].astype(BF16)
                for number in range(ways - 1):
                    outgoing_table(number).start()
                own_table().start()

            lax.fori_loop(0, ways, lambda d, c: (pack(s, h, d), c)[1], 0)
            for number in range(ways - 1):
                outgoing(s, h, number).start()
            own_block(s, h).start()
            return carry

        lax.fori_loop(0, groups, one_group, 0)
        return carry

    lax.fori_loop(0, streams, one_stream, 0)

    @pl.when(me < ways - 1)
    def _():
        for s in range(streams):
            pass_on(s).wait_send()

    for number in range(ways - 1):
        outgoing_table(number).wait_send()
        incoming_table(number).wait_recv()
    own_table().wait()
    scales = scales_ref[...]
    factors_ref[...] = factors_of(frames, scales, streams - 1)
    for s in range(streams):
        factors = factors_of(frames, scales, s)
        for h in range(groups):
            for number in range(ways - 1):
                outgoing(s, h, number).wait_send()
                incoming(s, h, number).wait_recv()
            own_block(s, h).wait()
            if (s, h) == (streams - 1, groups - 1):
                break
            target = early_ref.at[s] if s < streams - 1 else late_ref

            def decode_part(n, factors, s=s, h=h, target=target):
                for j in range(PART_ROWS):
                    decode_row(ways, got_ref.at[s, h], target, n * PART_ROWS + j, j, h * GROUP, factors[h * GROUP : (h + 1) * GROUP])
                return pltpu.roll(factors, LANES - PART_ROWS, 1)

            lax.fori_loop(0, own // PART_ROWS, decode_part, factors)


def factors_of(frames, scales, s):
    ways, own, _ = scales.shape
    table = scales.reshape(ways * own, LANES).astype(F32).T
    largest, ratio = table[2 * FIRST * s : 2 * FIRST * s + FIRST], table[2 * FIRST * s + FIRST : 2 * FIRST * (s + 1)]
    ratio = jnp.exp2(jnp.log(ratio) * np.float32(LOG2_E / POWER_SPAN) + np.float32(POWER_MID))
    power = largest * largest * ratio
    step = LANES // 2
    while step >= own:
        power = power + pltpu.roll(power, step, 1)
        step //= 2
    mean = power * np.float32(1.0 / (frames * ways))
    return largest * np.float32(LOG2_E / SPAN) * lax.rsqrt(mean + 1.0)


def decode_row(ways, got, out, j, column, row, factors):
    own = LANES // ways
    start = j * GROUP
    start = start if isinstance(start, int) else pl.multiple_of(start, GROUP)
    for way in range(ways):
        at = way * own + column
        for part in range(2):
            value = jnp.log(got[way, part, pl.ds(start, GROUP), :].astype(F32))
            out[part, j, row : row + GROUP, way * LANES : (way + 1) * LANES] = value * factors[:, at : at + 1]


def equalize(streams, ways, got_ref, factors_ref, early_ref, late_ref, out_ref, last_ref, early_sem, late_sem, last_sem):
    own = LANES // ways
    s, h = streams - 1, FIRST // GROUP - 1

    def copy_early(n):
        return pltpu.make_async_copy(early_ref.at[n], out_ref.at[n], early_sem.at[n])

    def copy_late():
        return pltpu.make_async_copy(late_ref, out_ref.at[s, :, :, pl.ds(0, h * GROUP), :], late_sem.at[0])

    def copy_last(n):
        rows = pl.ds(n * PART_ROWS, PART_ROWS)
        return pltpu.make_async_copy(
            last_ref.at[:, rows], out_ref.at[s, :, rows, pl.ds(h * GROUP, GROUP), :], last_sem.at[n]
        )

    for n in range(s):
        copy_early(n).start()
    copy_late().start()
    factors = factors_ref[h * GROUP :, :]
    for n in range(own // PART_ROWS):
        for j in range(n * PART_ROWS, (n + 1) * PART_ROWS):
            decode_row(ways, got_ref.at[s, h], last_ref, j, j, 0, factors)
        copy_last(n).start()
    for n in range(s):
        copy_early(n).wait()
    copy_late().wait()
    for n in range(own // PART_ROWS):
        copy_last(n).wait()


def shards(signal, taps):
    streams, _, samples = signal.shape
    channels = taps.shape[1]
    ways = lax.axis_size("tm")
    frames = samples // channels
    rows = 2 * FIRST
    own = LANES // ways
    z = signal.reshape(streams, 2, samples // LANES, LANES).transpose(0, 2, 1, 3).reshape(streams, frames * rows, LANES)
    constants = constant_table()
    vmem = pl.BlockSpec(memory_space=pltpu.VMEM)
    hbm = pl.BlockSpec(memory_space=pltpu.HBM)
    stay = pltpu.with_memory_space_constraint
    groups = FIRST // GROUP
    dma = pltpu.SemaphoreType.DMA
    share = channels // ways
    got, factors, early, late = pl.pallas_call(
        lambda *refs: channelize(streams, frames, ways, *refs),
        out_shape=(
            jax.ShapeDtypeStruct((streams, groups, ways, 2, own * GROUP, LANES), BF16),
            jax.ShapeDtypeStruct((FIRST, LANES), F32),
            jax.ShapeDtypeStruct((streams - 1, 2, own, FIRST, frames * ways), F32),
            jax.ShapeDtypeStruct((2, own, FIRST - GROUP, frames * ways), F32),
        ),
        in_specs=[hbm] * 3,
        out_specs=(vmem, vmem, vmem, vmem),
        scratch_shapes=[
            pltpu.VMEM((ways, own, LANES), BF16),
            pltpu.VMEM(taps.shape, F32),
            pltpu.VMEM(constants.shape, F32),
            pltpu.VMEM((4 * LANES, 2 * LANES), BF16),
            pltpu.VMEM((streams, (frames + 16) * rows, LANES), BF16),
            pltpu.VMEM((17 * TAPS_PITCH, LANES), F32),
            pltpu.VMEM((18 * FRAME_PITCH, LANES), F32),
            pltpu.VMEM((FIRST, frames, 2 * LANES), F32),
            pltpu.VMEM((2, (LANES + 1) * GROUP, LANES), F32),
            pltpu.VMEM((streams, groups, ways, 2, own * GROUP, LANES), BF16),
            pltpu.VMEM((LANES, LANES), F32),
            pltpu.VMEM((LANES, LANES), BF16),
            dma((2,)),
            dma((streams,)),
            dma((streams,)),
            dma((streams,)),
            dma((streams, groups, ways)),
            dma((streams, groups, ways)),
            dma((ways,)),
            dma((ways,)),
            dma((streams, groups)),
            dma((1,)),
        ],
        compiler_params=pltpu.CompilerParams(collective_id=0, has_side_effects=True, vmem_limit_bytes=40 << 20),
        name="channelize",
    )(stay(z, pltpu.HBM), stay(taps, pltpu.HBM), stay(jnp.asarray(constants), pltpu.HBM))
    out = pl.pallas_call(
        lambda *refs: equalize(streams, ways, *refs),
        out_shape=jax.ShapeDtypeStruct((streams, 2, own, FIRST, frames * ways), F32),
        in_specs=[vmem, vmem, vmem, vmem],
        out_specs=hbm,
        scratch_shapes=[
            pltpu.VMEM((2, own, GROUP, frames * ways), F32),
            dma((streams - 1,)),
            dma((1,)),
            dma((own // PART_ROWS,)),
        ],
        compiler_params=pltpu.CompilerParams(vmem_limit_bytes=16 << 20),
        name="equalize",
    )(got, factors, early, late)
    return out.reshape(streams, 2, share, frames * ways)


def solution(mesh):
    in_specs = (P("stream", None, "tm"), P())
    out_specs = P("stream", None, "tm", None)
    return jax.shard_map(shards, mesh=mesh, in_specs=in_specs, out_specs=out_specs, check_vma=False)
```
